32 devices in a mesh: dp: 8 (over y, x, core), tm: 4 (over z).
Axes of the slice: x: 2, y: 2, z: 4, core: 2. Of those that a mesh axis runs over, the one named last changes fastest.
Arguments:
- tokens: bfloat16 [8, 4, 256, 1024], P('dp', 'tm'), may hold values from -6 to 6
- gain: bfloat16 [1024], replicated, may hold values from 0.25 to 1.75
- w_qkv: bfloat16 [1024, 3072], P('dp'), may hold values from -0.1875 to 0.1875
- w_out: bfloat16 [1024, 1024], P('dp'), may hold values from -0.1875 to 0.1875
- w_pair: float32 [2, 1024, 32], replicated, may hold values from -3 to 3
- codebook: float32 [8, 32], replicated, may hold values from -5 to 5
- codes: int32 [8, 4, 1], P('dp', 'tm'), may hold values from 0 to 7
Outputs:
- grad_tokens: bfloat16 [8, 4, 256, 1024], P('dp', 'tm')
- grad_pair: float32 [2, 1024, 32], replicated
- codebook_step: float32 [8, 32], replicated
The draws below stay inside these ranges and needn't reach their ends.
Inputs may be any that keep to these rules, and one draw needn't show every extreme that they name: Every one of the 8 codes is assigned to some clip frame.
All inputs are finite; a program needn't handle non-finite values.
Results may differ from the reference program's by a relative error of at most 0.014.
Values may be sent and summed in bfloat16 or wider, within the bound.
A program may use at most 64 MiB of HBM per device.

```python
import jax
import jax.numpy as jnp
from jax import lax

D = 1024
HEAD_DIM = 64
LATENT = 32
CODES = 8
PATCHES = 256
CLIPS = 8
FRAMES = 4


def levels(rng, dims, pieces, least, top_value):
    loudness, own = 1.0, jax.random.fold_in(rng, 6)
    for dim, blocks in pieces:
        heights = jnp.exp(jax.random.uniform(jax.random.fold_in(own, dim), (blocks,), jnp.float32, least / len(pieces), top_value / len(pieces)))
        loudness = loudness * jnp.repeat(heights, dims[dim] // blocks).reshape([-1 if axis == dim else 1 for axis in range(len(dims))])
    return loudness


def distinct(key, rows, number_of, top, lift):
    ranking = jax.random.permutation(jax.random.fold_in(key, 1), number_of)
    favour = ranking
    for power in range(3):
        favour = favour * favour // number_of
    favour = favour * lift // number_of
    chance = jax.random.randint(jax.random.fold_in(key, 2), (rows, number_of), 0, 4096) + favour
    holders = jax.random.permutation(jax.random.fold_in(key, 3), rows)[jnp.arange(number_of) % rows]
    chance = jnp.where(jnp.arange(rows)[:, None] == holders[None, :], 1 << 14, chance)
    priority = chance * number_of + jnp.arange(number_of)
    return lax.top_k(priority.astype(jnp.int32), top)[1].astype(jnp.int32)


def scatter_about(own_key, dims, scale, bound, split=(), held_as=jnp.bfloat16):
    result = scale * jax.random.normal(own_key, dims, jnp.float32)
    if split:
        result = result * levels(own_key, dims, split, -0.22, 0.18)
    return jnp.clip(result, -bound, bound).astype(held_as)


def setup_inputs(seed: int = 0) -> dict:
    splits = jax.random.split(jax.random.key(seed), 8)
    return {
        "tokens": scatter_about(splits[0], (CLIPS, FRAMES, PATCHES, D), 1.0, 6.0, ((0, 8), (1, 4))),
        "gain": jnp.clip(1.0 + 0.15 * jax.random.normal(splits[1], (D,), jnp.float32), 0.25, 1.75).astype(jnp.bfloat16),
        "w_qkv": scatter_about(splits[2], (D, 3 * D), D ** -0.5, 0.1875, ((0, 8),)),
        "w_out": scatter_about(splits[3], (D, D), D ** -0.5, 0.1875, ((0, 8),)),
        "w_pair": scatter_about(splits[4], (2, D, LATENT), (D // PATCHES) ** -0.5, 3.0, (), jnp.float32),
        "codebook": scatter_about(splits[5], (CODES, LATENT), 1.0, 5.0, (), jnp.float32),
        "codes": distinct(splits[6], CLIPS * FRAMES, CODES, 1, 1024).reshape((CLIPS, FRAMES, 1)),
    }


EPS = 1e-06
BETA = 0.25

def normalize(xf, gain):
    scale = lax.rsqrt(lax.optimization_barrier(jnp.mean(xf * xf, axis=-1, keepdims=True)) + EPS)
    return (xf * scale * gain.astype(jnp.float32)).astype(jnp.bfloat16)

def project(normed, weight):
    shape = normed.shape
    flat = jnp.dot(normed.reshape(-1, shape[-1]), weight, preferred_element_type=jnp.float32)
    return flat.astype(jnp.bfloat16).reshape(shape[:-1] + (3, shape[-1]))

def attend(qkv):
    clips, frames, patches, _, width = qkv.shape
    local_heads = width // HEAD_DIM
    parts = qkv.reshape(clips, frames, patches, 3, local_heads, HEAD_DIM)
    query = parts[:, :, :, 0].astype(jnp.float32)
    keys = parts[:, :, :, 1].astype(jnp.float32)
    values = parts[:, :, :, 2].astype(jnp.float32)
    scores = jnp.einsum('cfphd,cgphd->cphfg', query, keys) * HEAD_DIM ** (-0.5)
    causal = jnp.arange(frames)[:, None] >= jnp.arange(frames)[None, :]
    scores = jnp.where(causal, scores, -1e+30)
    weights = jax.nn.softmax(scores, axis=-1).astype(jnp.bfloat16)
    mixed = jnp.einsum('cphfg,cgphd->cfphd', weights.astype(jnp.float32), values)
    return mixed.reshape(clips, frames, patches, width).astype(jnp.bfloat16)

def output(xf, attended, weight):
    shape = xf.shape
    moved = jnp.dot(attended.reshape(-1, shape[-1]), weight, preferred_element_type=jnp.float32)
    return lax.optimization_barrier(jnp.mean(xf + moved.reshape(shape), axis=2))

def reference(tokens, gain, w_qkv, w_out, w_pair, codebook, codes):

    def whole(xf):
        return output(xf, attend(project(normalize(xf, gain), w_qkv)), w_out)

    def forward(clip):
        return whole(clip[None].astype(jnp.float32))[0]
    pooled = lax.map(forward, tokens)
    following = jnp.concatenate([pooled[:, 1:], jnp.zeros_like(pooled[:, :1])], axis=1)
    flat_now = pooled.reshape(-1, D)
    flat_next = following.reshape(-1, D)
    hp = lax.Precision.HIGHEST
    action = jnp.dot(flat_now, w_pair[0], precision=hp) + jnp.dot(flat_next, w_pair[1], precision=hp)
    onehot = (codes.reshape(-1)[:, None] == jnp.arange(CODES)[None, :]).astype(jnp.float32)
    quantized = jnp.dot(onehot, codebook, precision=hp)
    diff = action - quantized
    d_action = 2.0 * BETA * diff
    d_quant = -2.0 * diff
    count = lax.optimization_barrier(jnp.sum(onehot, axis=0))
    codebook_step = jnp.dot(onehot.T, d_quant, precision=hp) / count[:, None]
    grad_pair = jnp.stack([jnp.dot(flat_now.T, d_action, precision=hp), jnp.dot(flat_next.T, d_action, precision=hp)])
    d_own = jnp.dot(d_action, w_pair[0].T, precision=hp).reshape(pooled.shape)
    d_next = jnp.dot(d_action, w_pair[1].T, precision=hp).reshape(pooled.shape)
    carried = jnp.concatenate([jnp.zeros_like(d_next[:, :1]), d_next[:, :-1]], axis=1)
    d_pooled = (d_own + carried) * PATCHES

    def backward(pair):
        clip, cotangent = pair
        _, pull = jax.vjp(whole, clip[None].astype(jnp.float32))
        return pull(cotangent[None])[0][0].astype(jnp.bfloat16)
    grad_tokens = lax.map(backward, (tokens, d_pooled))
    return (grad_tokens, grad_pair, codebook_step)
```

```python
import functools

import jax
import jax.numpy as jnp
from jax import lax
from jax.experimental import pallas as pl
from jax.experimental.pallas import tpu as pltpu
from jax.sharding import PartitionSpec as P

HEAD_DIM = 64
EPS = 1e-06
BETA = 0.25
LANES = 128
F32 = jnp.float32
BF16 = jnp.bfloat16
HIGH = lax.Precision.HIGHEST


def dot(a, b, ca=1, cb=0, precision=None):
    return lax.dot_general(
        a, b, (((ca,), (cb,)), ((), ())), precision=precision, preferred_element_type=F32
    )


def dot_split(a, b, cb=0):
    high = a.astype(BF16)
    rest = a - high.astype(F32)
    mid = rest.astype(BF16)
    low = (rest - mid.astype(F32)).astype(BF16)
    n = a.shape[0]
    terms = jnp.concatenate([high.astype(F32), mid.astype(F32), low.astype(F32)], axis=0)
    out = dot(terms.astype(BF16), b, 1, cb)
    return out[:n] + out[n : 2 * n] + out[2 * n :]


def bits_of(n):
    return max(n.bit_length() - 1, 0)


def ring_place(chip, n):
    b = [(chip // 2**k) % 2 for k in range(bits_of(n))]
    return sum(((sum(b[k:]) % 2) * 2**k for k in range(len(b))), 0)


def ring_chip(place, n):
    count = bits_of(n)
    b = [(place // 2**k) % 2 for k in range(count)] + [0]
    return sum((((b[k] + b[k + 1]) % 2) * 2**k for k in range(count)), 0)


def split2(a):
    high = a.astype(BF16).astype(F32)
    return high, a - high


def reduce_rows(v, parts, n):
    high, mid = split2(v)
    r = dot(jnp.concatenate([high, mid], axis=0).astype(BF16), parts[0 : 2 * n, :], 1, 1)
    r = r[: v.shape[0]] + r[v.shape[0] :]
    return r[:, :n] + r[:, n : 2 * n]


def expand_rows(b, parts):
    high, mid = split2(b)
    return dot(jnp.concatenate([high, high, mid], axis=1).astype(BF16), parts[...])


def three_parts(value):
    high, mid = split2(value)
    return jnp.concatenate([high, mid, high], axis=0).astype(BF16)


def kernel(
    cfg, tokens, gain_in, wq_own, wo_in, wp_in, codebook_in, codes_in,
    out, pair_out, step_out,
    wq, wo, wp, gain, codebook, codes, x, normed, scales, acc, qkv, place, lift,
    w_full, w_low, d_big, d_s, dqkv, dn, done, d_rows, d_att,
    wps, mts, mt_all, tile, tile_all, sums, sums_all, msg, msg_all, part, part_all, final_all,
    send, recv, local_sem,
):
    dp, tm, rows, patches, width, latent, n_codes, groups = cfg
    mine = patches // tm
    total = tm * mine
    sub = mine // groups
    part_rows = tm * sub
    fp, sr = tile.shape[0], sums.shape[0]
    heads = width // HEAD_DIM
    lanes = tm * heads
    both = 2 * latent
    chips = dp // 2
    half_ring = chips // 2
    i = lax.axis_index("dp")
    t = lax.axis_index("tm")
    core = i % 2
    spot = ring_place(i // 2, chips)

    def device_at(p, c):
        return ring_chip((p + 2 * chips) % chips, chips) * 2 + c

    barrier = pltpu.get_barrier_semaphore()
    for r in range(1, tm):
        pl.semaphore_signal(barrier, inc=1, device_id={"dp": i, "tm": (t + r) % tm})
    for r in range(1, dp):
        pl.semaphore_signal(barrier, inc=1, device_id={"dp": (i + r) % dp, "tm": t})

    def frame_rows(f):
        return pl.ds(pl.multiple_of(f * mine, mine), mine)

    here = [
        pltpu.make_async_copy(src, dst, local_sem.at[n])
        for n, (src, dst) in enumerate((
            (wq_own, wq.at[pl.ds(pl.multiple_of(i * rows, rows), rows)]),
            (wo_in, wo),
            (wp_in, wp),
            (gain_in, gain),
            (tokens.at[frame_rows(t)], x.at[frame_rows(t)]),
            (codebook_in, codebook),
            (codes_in, codes),
        ))
    ]
    for copy in here:
        copy.start()

    col_head = lax.broadcasted_iota(jnp.int32, (width, lanes), 0) // HEAD_DIM
    lane_id = lax.broadcasted_iota(jnp.int32, (width, lanes), 1)
    for f in range(tm):
        place[f * width : (f + 1) * width, :] = jnp.where(lane_id == f * heads + col_head, 1.0, 0.0).astype(BF16)
    row_head = lax.broadcasted_iota(jnp.int32, (lanes, width), 0) % heads
    lift_col = lax.broadcasted_iota(jnp.int32, (lanes, width), 1) // HEAD_DIM
    lift[...] = jnp.where(row_head == lift_col, 1.0, 0.0).astype(BF16)

    tags = {}

    def tag(*key):
        return tags.setdefault(key, len(tags))

    started = []

    def remote(src, dst, key, dpi, tmi):
        k = tag(*key)
        return pltpu.make_async_remote_copy(
            src_ref=src, dst_ref=dst, send_sem=send.at[k], recv_sem=recv.at[k],
            device_id={"dp": dpi, "tm": tmi},
        )

    def go(copy):
        copy.start()
        started.append(copy)

    half = rows // 2
    dirs = (1, -1)
    quarter = half // 2
    sharing = half_ring == 2 and quarter % 16 == 0 and tm % 2 == 0
    odd = t % 2
    twin = t + 1 - 2 * odd

    def piece(origin, h):
        return wq.at[pl.ds(pl.multiple_of(origin * rows + h * half, half), half)]

    def split(d, s, h):
        return sharing and s == 0 and h != main_half(d)

    def quarter_of(origin, h, which):
        at = origin * rows + h * half + which * quarter
        return wq.at[pl.ds(pl.multiple_of(at, quarter), quarter)]

    def main_half(d):
        return 0 if dirs[d] == 1 else 1

    def halves(d, s):
        first = main_half(d)
        return (first, 1 - first) if s < half_ring - 1 else (first,)

    def ring_copy(d, s, h):
        origin = device_at(spot - dirs[d] * s, core)
        ref = quarter_of(origin, h, odd) if split(d, s, h) else piece(origin, h)
        return remote(ref, ref, ("ring", d, s, h), device_at(spot + dirs[d], core), t)

    def sib_copy(d, s, h):
        ref = piece(device_at(spot - dirs[d] * s, core), h)
        return remote(ref, ref, ("sib", d, s, h), device_at(spot, 1 - core), t)

    def twin_copy(d):
        at = quarter_of(device_at(spot - dirs[d], core), 1 - main_half(d), odd)
        return remote(at, at, ("twin", d), i, twin)

    def quarter_sib(d, n):
        which = odd if n == 0 else 1 - odd
        at = quarter_of(device_at(spot - dirs[d], core), 1 - main_half(d), which)
        return remote(at, at, ("quarter", d, n), device_at(spot, 1 - core), t)

    def take(d, s, h):
        ring_copy(d, s, h).wait_recv()
        if split(d, s, h):
            go(twin_copy(d))
            go(quarter_sib(d, 0))
            return
        if s + 1 < half_ring and h in halves(d, s + 1):
            go(ring_copy(d, s + 1, h))
        go(sib_copy(d, s + 1, h))

    def map_copy(k):
        at = mt_all.at[device_at(spot - k, core)]
        if k == 0:
            return remote(at, at, ("map", 0), device_at(spot, 1 - core), t)
        return remote(at, at, ("map", k), device_at(spot, 1 - core), t)

    def map_far(k):
        return remote(mt_all.at[i], mt_all.at[i], ("far", k), device_at(spot + k, core), t)

    here[0].wait()
    pl.semaphore_wait(barrier, tm + dp - 2)
    for n in range(2):
        for d in range(2):
            if n < len(halves(d, 0)):
                go(ring_copy(d, 0, halves(d, 0)[n]))
    for r in sorted(range(1, tm), key=lambda r: -min(r, tm - r)):
        other = (t + r) % tm
        go(remote(tokens.at[frame_rows(other)], x.at[frame_rows(t)], ("tok", r), i, other))
    for h in range(2):
        go(sib_copy(0, 0, h))

    for copy in here[1:]:
        copy.wait()
    mt_all[i] = dot_split(wp[...], wo[...], 1)
    for k in range(1, chips):
        go(map_far(k))
    go(map_copy(0))
    wps[...] = three_parts(wp[...])

    if half_ring > 1:
        for d in range(2):
            take(d, 0, main_half(d))

    for r in range(1, tm):
        remote(tokens.at[frame_rows(t)], x.at[frame_rows(t)], ("tok", r), i, t).wait_recv()

    block = 32
    gain_row = gain[...].astype(F32).reshape(1, width)

    def norm_step(b, carry):
        at = pl.ds(pl.multiple_of(b * block, block), block)
        xf = x[at, :].astype(F32)
        scale = lax.rsqrt(jnp.mean(xf * xf, axis=-1, keepdims=True) + EPS)
        scales[at, :] = jnp.broadcast_to(scale, (block, LANES))
        normed[at, :] = (xf * scale * gain_row).astype(BF16)
        return carry

    lax.fori_loop(0, total // block, norm_step, 0)

    frow = lax.broadcasted_iota(jnp.int32, (fp, total), 0)
    fcol = lax.broadcasted_iota(jnp.int32, (fp, total), 1)
    x_sum = dot(jnp.where(fcol // mine == frow, 1.0, 0.0).astype(BF16), x[...])
    sums[...] = jnp.zeros_like(sums)
    sums[tm : 2 * tm, :] = x_sum[:tm]
    trow = lax.broadcasted_iota(jnp.int32, (fp, LANES), 0)
    tlane = lax.broadcasted_iota(jnp.int32, (fp, LANES), 1)
    tile[...] = jnp.where((trow == t) & (tlane == both + codes[0, 0]), 1.0, 0.0).astype(F32)
    x_part = reduce_rows(x_sum, wps, both)

    for k in range(1, chips):
        remote(mt_all.at[i], mt_all.at[i], ("far", k), i, t).wait_recv()
        go(map_copy(k))

    pair = 2 * rows
    columns = 512

    def project(p, first, last):
        base = pl.multiple_of(ring_chip((p + 2 * chips) % chips, chips) * pair, pair)

        def body(n, carry):
            at = pl.ds(pl.multiple_of(n * columns, columns), columns)
            got = dot(normed[:, pl.ds(base, pair)], wq[pl.ds(base, pair), at])
            if not first:
                got = got + acc[:, at]
            if last:
                qkv[:, at] = got.astype(BF16)
            else:
                acc[:, at] = got
            return carry

        lax.fori_loop(0, 3 * width // columns, body, 0)

    def wait_sib(d, s, h):
        sib_copy(d, s, h).wait_recv()

    by_chip = pair % LANES == 0
    for h in range(2):
        wait_sib(0, 0, h)
    if by_chip:
        project(spot, True, chips == 1)
    if sharing:
        for d in range(2):
            take(d, 0, 1 - main_half(d))
        for d in range(2):
            twin_copy(d).wait_recv()
            go(quarter_sib(d, 1))
        for d in range(2):
            wait_sib(d, 1, main_half(d))
            for n in range(2):
                quarter_sib(d, n).wait_recv()
            if by_chip:
                project(spot - dirs[d], False, False)
            if d == 0:
                for e in range(2):
                    take(e, 1, main_half(e))
    else:
        for s in range(half_ring):
            for d in range(2):
                for n, h in enumerate(halves(d, s)):
                    if not (half_ring > 1 and s == 0 and n == 0):
                        take(d, s, h)
            if s < half_ring - 1:
                for d in range(2):
                    for h in halves(d, s):
                        wait_sib(d, s + 1, h)
                    if by_chip:
                        project(spot - dirs[d] * (s + 1), False, False)

    for k in range(chips):
        map_copy(k).wait_recv()
    mts[...] = three_parts(jnp.concatenate([mt_all[n] for n in range(dp)], axis=1))

    for d in range(2):
        for h in halves(d, half_ring - 1):
            wait_sib(d, half_ring, h)
    if by_chip:
        project(spot + half_ring, False, True)
    else:
        def whole_body(n, carry):
            at = pl.ds(pl.multiple_of(n * columns, columns), columns)
            qkv[:, at] = dot(normed[...], wq[:, at]).astype(BF16)
            return carry

        lax.fori_loop(0, 3 * width // columns, whole_body, 0)

    scale_q = HEAD_DIM ** (-0.5)

    def frame(f):
        return slice(f * mine, (f + 1) * mine)

    scores = [None] * tm
    for f in range(tm):
        q = qkv[frame(f), 0:width]
        products = jnp.concatenate([q] * (f + 1), axis=0) * qkv[0 : (f + 1) * mine, width : 2 * width]
        r = dot(products, place[f * width : (f + 1) * width, :])
        for g in range(f + 1):
            scores[g] = r[frame(g)] if scores[g] is None else scores[g] + r[frame(g)]
    lane_frame = lax.broadcasted_iota(jnp.int32, (mine, lanes), 1) // heads
    scores = [jnp.where(lane_frame >= g, s * scale_q, -1e30) for g, s in enumerate(scores)]
    top = functools.reduce(jnp.maximum, scores)
    raised = [jnp.exp(s - top) for s in scores]
    whole = functools.reduce(jnp.add, raised)
    for g in range(tm):
        w = raised[g] / whole
        w_full[frame(g), :] = w
        w_low[frame(g), :] = w.astype(BF16)
    mixed = dot(w_low[...], qkv[:, 2 * width :], 0, 0) * lift[...].astype(F32)
    sums[0:tm, :] = jnp.sum(mixed.reshape(tm, heads, width), axis=1)

    tile[:, :both] = (reduce_rows(sums[0:fp, :], mts, both) + x_part) * (1.0 / patches)
    for r in range(1, tm):
        go(remote(tile, tile_all.at[t], ("tile", r), i, (t + r) % tm))
    for r in range(1, tm):
        go(remote(sums, sums_all.at[t], ("sum", r), i, (t + r) % tm))
    tile_all[t] = tile[...]
    sums_all[t] = sums[...]
    for r in range(1, tm):
        remote(tile, tile_all.at[t], ("tile", r), i, t).wait_recv()

    tot = tile_all[0]
    for r in range(1, tm):
        tot = tot + tile_all[r]
    lrow = lax.broadcasted_iota(jnp.int32, (fp, latent), 0)
    following = jnp.where(lrow < tm - 1, pltpu.roll(tot, fp - 1, 0)[:, latent:both], 0.0)
    onehot = tot[:, both : both + n_codes]
    quantized = onehot[:, 0:1] * codebook[0:1, :]
    for n in range(1, n_codes):
        quantized = quantized + onehot[:, n : n + 1] * codebook[n : n + 1, :]
    d_action = jnp.where(lrow < tm, (2.0 * BETA) * (tot[:, :latent] + following - quantized), 0.0)
    earlier = jnp.where((lrow > 0) & (lrow < tm), pltpu.roll(d_action, 1, 0), 0.0)
    d_pair = jnp.concatenate([d_action, earlier], axis=1)
    d_att[...] = expand_rows(d_pair, mts).astype(BF16).astype(F32)
    d_rows[...] = expand_rows(d_pair, wps)

    for f in range(tm):
        at = slice(f * heads, (f + 1) * heads)
        d_big[at, :] = (lift[at, :].astype(F32) * d_att[f : f + 1, :]).astype(BF16)
    d_w = dot(qkv[:, 2 * width :], d_big[...], 1, 1).astype(BF16).astype(F32)
    wd = [w_full[frame(g), :] * d_w[frame(g)] for g in range(tm)]
    mean = functools.reduce(jnp.add, wd)
    for g in range(tm):
        d_s[frame(g), :] = ((wd[g] - w_full[frame(g), :] * mean) * scale_q).astype(BF16).astype(F32)

    wide = 256

    def backward(n):
        def own(f):
            return slice(f * mine + n * sub, f * mine + (n + 1) * sub)

        def at(f):
            return slice(n * part_rows + f * sub, n * part_rows + (f + 1) * sub)

        lane_f = lax.broadcasted_iota(jnp.int32, (sub, lanes), 1) // heads
        picked = [
            jnp.concatenate([jnp.where(lane_f == f, d_s[own(g), :], 0.0) for g in range(f + 1)], axis=0).astype(BF16)
            for f in range(tm)
        ]
        for c in range(0, width, wide):
            k = [qkv[own(g), width + c : width + c + wide].astype(F32) for g in range(tm)]
            dk = [None] * tm
            for f in range(tm):
                q = qkv[own(f), c : c + wide].astype(F32)
                spread = dot(picked[f], lift[:, c : c + wide])
                dq = None
                for g in range(f + 1):
                    s = spread[g * sub : (g + 1) * sub]
                    dq = s * k[g] if dq is None else dq + s * k[g]
                    dk[g] = s * q if dk[g] is None else dk[g] + s * q
                dqkv[at(f), c : c + wide] = dq.astype(BF16)
            for g in range(tm):
                dqkv[at(g), width + c : width + c + wide] = dk[g].astype(BF16)
        low = jnp.concatenate([w_low[own(g), :] for g in range(tm)], axis=0)
        group = slice(n * part_rows, (n + 1) * part_rows)
        dqkv[group, 2 * width :] = dot(low, d_big[...]).astype(BF16)
        for c in range(0, width, 512):
            dn[:, c : c + 512] = dot(dqkv[group, :], wq[c : c + 512, :], 1, 1).astype(BF16)
        for f in range(tm):
            xf = x[own(f), :].astype(F32)
            scale = scales[own(f), 0:1]
            u = dn[f * sub : (f + 1) * sub, :].astype(F32) * gain_row
            inner = jnp.mean(xf * u, axis=-1, keepdims=True)
            dx = u * scale - xf * (scale * scale * scale * inner)
            done[at(f), :] = (d_rows[f : f + 1, :] + dx).astype(BF16)

    def done_copy(n, r, other):
        return remote(
            done.at[pl.ds(pl.multiple_of(n * part_rows + other * sub, sub), sub)],
            out.at[pl.ds(pl.multiple_of(t * mine + n * sub, sub), sub)], ("done", n, r), i, other,
        )

    def give(n):
        for r in sorted(range(1, tm), key=lambda r: -min(r, tm - r)):
            go(done_copy(n, r, (t + r) % tm))
        out[pl.ds(pl.multiple_of(t * mine + n * sub, sub), sub), :] = done[
            pl.ds(pl.multiple_of(n * part_rows + t * sub, sub), sub), :
        ]

    def share():
        for r in range(1, tm):
            remote(sums, sums_all.at[t], ("sum", r), i, t).wait_recv()
        s = sums_all[0]
        for r in range(1, tm):
            s = s + sums_all[r]
        s = s * (1.0 / patches)
        blank = jnp.zeros((sr, LANES), F32)
        for n in range(dp):
            msg[n] = jnp.zeros_like(msg[n])
            msg[n, 0, :, 0:rows] = s[:, n * rows : (n + 1) * rows]
            msg[n, 1, 0:tm, 0:both] = d_pair[:tm]
            msg[n, 1, tm : 2 * tm, both : 2 * both] = d_pair[:tm]
            msg[n, 2, 0:tm, 0:both] = d_pair[:tm]
            msg[n, 2, 0:tm, both : both + n_codes] = onehot[:tm]
        for r in range(1, dp):
            other = (i + r) % dp
            go(remote(msg.at[other], msg_all.at[i], ("msg", r), other, t))
        msg_all[i] = msg[i]

    for n in range(groups):
        backward(n)
        give(n)
        if n == 0:
            share()

    for r in range(1, dp):
        remote(msg.at[i], msg_all.at[i], ("msg", r), i, t).wait_recv()
    every = dp * sr
    slices = msg_all[:, 0].reshape(every, LANES)
    cross = dot(msg_all[:, 1].reshape(every, LANES), slices, 0, 0, precision=HIGH)
    mapped = dot_split(cross[:both, :rows], wo[...])
    for n in range(dp):
        part[n] = mapped[:, n * rows : (n + 1) * rows]
    for r in range(1, dp):
        other = (i + r) % dp
        go(remote(part.at[other], part_all.at[i], ("part", r), other, t))
    part_all[i] = part[i] + cross[both : 2 * both, :rows]
    marks = msg_all[:, 2].reshape(every, LANES)
    table = dot(marks, marks, 0, 0, precision=HIGH)[both : both + n_codes]
    count = jnp.sum(table[:, both : both + n_codes], axis=1, keepdims=True)
    step_out[...] = table[:, :latent] * (-1.0 / BETA) / count

    for r in range(1, dp):
        remote(part.at[i], part_all.at[i], ("part", r), i, t).wait_recv()
    final = part_all[0]
    for n in range(1, dp):
        final = final + part_all[n]
    final_all[i] = final
    for r in range(1, dp):
        go(remote(final_all.at[i], final_all.at[i], ("final", r), (i + r) % dp, t))
    for r in range(1, dp):
        remote(final_all.at[i], final_all.at[i], ("final", r), i, t).wait_recv()
    for n in range(dp):
        for m in range(2):
            pair_out[m, :, n * rows : (n + 1) * rows] = final_all[n, m * latent : (m + 1) * latent, :]

    for n in range(groups):
        for r in range(1, tm):
            done_copy(n, r, t).wait_recv()
    for copy in started:
        copy.wait_send()
    assert len(tags) <= send.shape[0]


def local(dp, tm, tokens, gain, w_qkv, w_out, w_pair, codebook, codes):
    patches, width = tokens.shape[2:]
    rows = w_qkv.shape[0]
    latent, n_codes = w_pair.shape[2], codebook.shape[0]
    both = 2 * latent
    fp = -(-tm // 8) * 8
    sr = -(-2 * tm // 8) * 8
    lanes = tm * (width // HEAD_DIM)
    groups = 2 if patches // tm % 32 == 0 else 1
    part_rows = patches // groups
    assert rows <= LANES and 2 * both <= LANES and both + n_codes <= LANES
    tags = (tm - 1) * (3 + groups) + 3 * (dp - 1) + 5 * dp + 16
    vmem = pl.BlockSpec(memory_space=pltpu.VMEM)
    hbm = pl.BlockSpec(memory_space=pltpu.HBM)
    grad, pair, step = pl.pallas_call(
        functools.partial(kernel, (dp, tm, rows, patches, width, latent, n_codes, groups)),
        out_shape=(
            jax.ShapeDtypeStruct((patches, width), BF16),
            jax.ShapeDtypeStruct((2, latent, width), F32),
            jax.ShapeDtypeStruct((n_codes, latent), F32),
        ),
        in_specs=[hbm] * 7,
        out_specs=(vmem, vmem, vmem),
        scratch_shapes=[
            pltpu.VMEM((dp * rows, 3 * width), BF16),
            pltpu.VMEM((rows, width), BF16),
            pltpu.VMEM((both, width), F32),
            pltpu.VMEM((width,), BF16),
            pltpu.VMEM((n_codes, latent), F32),
            pltpu.SMEM((1, 1), jnp.int32),
            pltpu.VMEM((patches, width), BF16),
            pltpu.VMEM((patches, width), BF16),
            pltpu.VMEM((patches, LANES), F32),
            pltpu.VMEM((patches, 3 * width), F32),
            pltpu.VMEM((patches, 3 * width), BF16),
            pltpu.VMEM((tm * width, lanes), BF16),
            pltpu.VMEM((lanes, width), BF16),
            pltpu.VMEM((patches, lanes), F32),
            pltpu.VMEM((patches, lanes), BF16),
            pltpu.VMEM((lanes, width), BF16),
            pltpu.VMEM((patches, lanes), F32),
            pltpu.VMEM((patches, 3 * width), BF16),
            pltpu.VMEM((part_rows, width), BF16),
            pltpu.VMEM((patches, width), BF16),
            pltpu.VMEM((fp, width), F32),
            pltpu.VMEM((fp, width), F32),
            pltpu.VMEM((3 * both, width), BF16),
            pltpu.VMEM((3 * both, width), BF16),
            pltpu.VMEM((dp, both, rows), F32),
            pltpu.VMEM((fp, LANES), F32),
            pltpu.VMEM((tm, fp, LANES), F32),
            pltpu.VMEM((sr, width), F32),
            pltpu.VMEM((tm, sr, width), F32),
            pltpu.VMEM((dp, 3, sr, LANES), F32),
            pltpu.VMEM((dp, 3, sr, LANES), F32),
            pltpu.VMEM((dp, both, rows), F32),
            pltpu.VMEM((dp, both, rows), F32),
            pltpu.VMEM((dp, both, rows), F32),
            pltpu.SemaphoreType.DMA((tags,)),
            pltpu.SemaphoreType.DMA((tags,)),
            pltpu.SemaphoreType.DMA((7,)),
        ],
        compiler_params=pltpu.CompilerParams(
            collective_id=0, has_side_effects=True, vmem_limit_bytes=44000 * 1024
        ),
    )(
        tokens.reshape(patches, width), gain, w_qkv, w_out, w_pair.swapaxes(1, 2).reshape(both, width), codebook,
        codes.reshape(1, 1),
    )
    return grad.reshape(tokens.shape), pair.swapaxes(1, 2), step


def solution(mesh):
    placed = (
        P("dp", "tm", None, None),
        P(),
        P("dp", None),
        P("dp", None),
        P(),
        P(),
        P("dp", "tm", None),
    )
    return jax.shard_map(
        functools.partial(local, mesh.shape["dp"], mesh.shape["tm"]),
        mesh=mesh,
        in_specs=placed,
        out_specs=(P("dp", "tm", None, None), P(), P()),
        check_vma=False,
    )
```

```python
import functools

import jax
import jax.numpy as jnp
from jax import lax
from jax.experimental import pallas as pl
from jax.experimental.pallas import tpu as pltpu
from jax.sharding import PartitionSpec as P

HEAD_DIM = 64
EPS = 1e-06
BETA = 0.25
LANES = 128
F32 = jnp.float32
BF16 = jnp.bfloat16
HIGH = lax.Precision.HIGHEST


def dot(a, b, ca=1, cb=0, precision=None):
    return lax.dot_general(
        a, b, (((ca,), (cb,)), ((), ())), precision=precision, preferred_element_type=F32
    )


def dot_split(a, b, cb=0):
    high = a.astype(BF16)
    rest = a - high.astype(F32)
    mid = rest.astype(BF16)
    low = (rest - mid.astype(F32)).astype(BF16)
    n = a.shape[0]
    terms = jnp.concatenate([high.astype(F32), mid.astype(F32), low.astype(F32)], axis=0)
    out = dot(terms.astype(BF16), b, 1, cb)
    return out[:n] + out[n : 2 * n] + out[2 * n :]


def bits_of(n):
    return max(n.bit_length() - 1, 0)


def ring_place(chip, n):
    b = [(chip // 2**k) % 2 for k in range(bits_of(n))]
    return sum(((sum(b[k:]) % 2) * 2**k for k in range(len(b))), 0)


def ring_chip(place, n):
    count = bits_of(n)
    b = [(place // 2**k) % 2 for k in range(count)] + [0]
    return sum((((b[k] + b[k + 1]) % 2) * 2**k for k in range(count)), 0)


def split2(a):
    high = a.astype(BF16).astype(F32)
    return high, a - high


def reduce_rows(v, parts, n):
    high, mid = split2(v)
    r = dot(jnp.concatenate([high, mid], axis=0).astype(BF16), parts[0 : 2 * n, :], 1, 1)
    r = r[: v.shape[0]] + r[v.shape[0] :]
    return r[:, :n] + r[:, n : 2 * n]


def expand_rows(b, parts):
    high, mid = split2(b)
    return dot(jnp.concatenate([high, high, mid], axis=1).astype(BF16), parts[...])


def three_parts(value):
    high, mid = split2(value)
    return jnp.concatenate([high, mid, high], axis=0).astype(BF16)


def kernel(
    cfg, tokens, gain_in, wq_own, wo_in, wp_in, codebook_in, codes_in,
    out, pair_out, step_out,
    wq, wo, wp, gain, codebook, codes, x, normed, scales, acc, qkv, place, lift,
    w_full, w_low, d_big, d_s, dqkv, dn, done, d_rows, d_att,
    wps, mts, mt_all, tile, tile_all, sums, sums_all, msg, msg_all, part, part_all, final_all,
    send, recv, local_sem,
):
    dp, tm, rows, patches, width, latent, n_codes, groups = cfg
    mine = patches // tm
    total = tm * mine
    sub = mine // groups
    part_rows = tm * sub
    fp, sr = tile.shape[0], sums.shape[0]
    heads = width // HEAD_DIM
    lanes = tm * heads
    both = 2 * latent
    chips = dp // 2
    half_ring = chips // 2
    i = lax.axis_index("dp")
    t = lax.axis_index("tm")
    core = i % 2
    spot = ring_place(i // 2, chips)

    def device_at(p, c):
        return ring_chip((p + 2 * chips) % chips, chips) * 2 + c

    barrier = pltpu.get_barrier_semaphore()
    for r in range(1, tm):
        pl.semaphore_signal(barrier, inc=1, device_id={"dp": i, "tm": (t + r) % tm})
    for r in range(1, dp):
        pl.semaphore_signal(barrier, inc=1, device_id={"dp": (i + r) % dp, "tm": t})

    def frame_rows(f):
        return pl.ds(pl.multiple_of(f * mine, mine), mine)

    here = [
        pltpu.make_async_copy(src, dst, local_sem.at[n])
        for n, (src, dst) in enumerate((
            (wq_own, wq.at[pl.ds(pl.multiple_of(i * rows, rows), rows)]),
            (wo_in, wo),
            (wp_in, wp),
            (gain_in, gain),
            (tokens.at[frame_rows(t)], x.at[frame_rows(t)]),
            (codebook_in, codebook),
            (codes_in, codes),
        ))
    ]
    for copy in here:
        copy.start()

    col_head = lax.broadcasted_iota(jnp.int32, (width, lanes), 0) // HEAD_DIM
    lane_id = lax.broadcasted_iota(jnp.int32, (width, lanes), 1)
    for f in range(tm):
        place[f * width : (f + 1) * width, :] = jnp.where(lane_id == f * heads + col_head, 1.0, 0.0).astype(BF16)
    row_head = lax.broadcasted_iota(jnp.int32, (lanes, width), 0) % heads
    lift_col = lax.broadcasted_iota(jnp.int32, (lanes, width), 1) // HEAD_DIM
    lift[...] = jnp.where(row_head == lift_col, 1.0, 0.0).astype(BF16)

    tags = {}

    def tag(*key):
        return tags.setdefault(key, len(tags))

    started = []

    def remote(src, dst, key, dpi, tmi):
        k = tag(*key)
        return pltpu.make_async_remote_copy(
            src_ref=src, dst_ref=dst, send_sem=send.at[k], recv_sem=recv.at[k],
            device_id={"dp": dpi, "tm": tmi},
        )

    def go(copy):
        copy.start()
        started.append(copy)

    half = rows // 2
    dirs = (1, -1)
    quarter = half // 2
    sharing = half_ring == 2 and quarter % 16 == 0 and tm % 2 == 0
    odd = t % 2
    twin = t + 1 - 2 * odd

    def piece(origin, h):
        return wq.at[pl.ds(pl.multiple_of(origin * rows + h * half, half), half)]

    def main_half(d):
        return 0 if dirs[d] == 1 else 1

    def halves(d, s):
        first = main_half(d)
        return (first, 1 - first) if s < half_ring - 1 else (first,)

    def quarter_of(origin, h, which):
        at = origin * rows + h * half + which * quarter
        return wq.at[pl.ds(pl.multiple_of(at, quarter), quarter)]

    def ring_copy(d, s, h):
        ref = piece(device_at(spot - dirs[d] * s, core), h)
        return remote(ref, ref, ("ring", d, s, h), device_at(spot + dirs[d], core), t)

    def sib_copy(d, s, h):
        ref = piece(device_at(spot - dirs[d] * s, core), h)
        return remote(ref, ref, ("sib", d, s, h), device_at(spot, 1 - core), t)

    def take(d, s, h):
        ring_copy(d, s, h).wait_recv()
        if s + 1 < half_ring and h in halves(d, s + 1):
            go(ring_copy(d, s + 1, h))
        go(sib_copy(d, s + 1, h))

    def shared_copy(d):
        ref = quarter_of(i, 1 - main_half(d), odd)
        return remote(ref, ref, ("shared", d), device_at(spot + dirs[d], core), t)

    def twin_copy(d):
        at = quarter_of(device_at(spot - dirs[d], core), 1 - main_half(d), odd)
        return remote(at, at, ("twin", d), i, twin)

    def quarter_sib(d, n):
        which = odd if n == 0 else 1 - odd
        at = quarter_of(device_at(spot - dirs[d], core), 1 - main_half(d), which)
        return remote(at, at, ("quarter", d, n), device_at(spot, 1 - core), t)

    def main_copy(d, s, n):
        ref = quarter_of(device_at(spot - dirs[d] * s, core), main_half(d), n)
        return remote(ref, ref, ("main", d, s, n), device_at(spot + dirs[d], core), t)

    def main_sib(d, s, n):
        ref = quarter_of(device_at(spot - dirs[d] * s, core), main_half(d), n)
        return remote(ref, ref, ("mainsib", d, s, n), device_at(spot, 1 - core), t)

    def take_main(d, s, n):
        main_copy(d, s, n).wait_recv()
        if s == 0:
            go(main_copy(d, 1, n))
        go(main_sib(d, s + 1, n))

    def map_copy(k):
        at = mt_all.at[device_at(spot - k, core)]
        if k == 0:
            return remote(at, at, ("map", 0), device_at(spot, 1 - core), t)
        return remote(at, at, ("map", k), device_at(spot, 1 - core), t)

    def map_far(k):
        return remote(mt_all.at[i], mt_all.at[i], ("far", k), device_at(spot + k, core), t)

    here[0].wait()
    pl.semaphore_wait(barrier, tm + dp - 2)
    if sharing:
        for d in range(2):
            go(shared_copy(d))
        for n in range(2):
            for d in range(2):
                go(main_copy(d, 0, n))
    else:
        for n in range(2):
            for d in range(2):
                if n < len(halves(d, 0)):
                    go(ring_copy(d, 0, halves(d, 0)[n]))
    for r in sorted(range(1, tm), key=lambda r: -min(r, tm - r)):
        other = (t + r) % tm
        go(remote(tokens.at[frame_rows(other)], x.at[frame_rows(t)], ("tok", r), i, other))
    for h in range(2):
        go(sib_copy(0, 0, h))

    for copy in here[1:]:
        copy.wait()
    mt_all[i] = dot_split(wp[...], wo[...], 1)
    for k in range(1, chips):
        go(map_far(k))
    go(map_copy(0))
    wps[...] = three_parts(wp[...])

    if sharing:
        for d in range(2):
            shared_copy(d).wait_recv()
            go(twin_copy(d))
            go(quarter_sib(d, 0))
        for n in range(2):
            for d in range(2):
                take_main(d, 0, n)
    elif half_ring > 1:
        for d in range(2):
            take(d, 0, main_half(d))

    for r in range(1, tm):
        remote(tokens.at[frame_rows(t)], x.at[frame_rows(t)], ("tok", r), i, t).wait_recv()

    block = 32
    gain_row = gain[...].astype(F32).reshape(1, width)

    def norm_step(b, carry):
        at = pl.ds(pl.multiple_of(b * block, block), block)
        xf = x[at, :].astype(F32)
        scale = lax.rsqrt(jnp.mean(xf * xf, axis=-1, keepdims=True) + EPS)
        scales[at, :] = jnp.broadcast_to(scale, (block, LANES))
        normed[at, :] = (xf * scale * gain_row).astype(BF16)
        return carry

    lax.fori_loop(0, total // block, norm_step, 0)

    frow = lax.broadcasted_iota(jnp.int32, (fp, total), 0)
    fcol = lax.broadcasted_iota(jnp.int32, (fp, total), 1)
    x_sum = dot(jnp.where(fcol // mine == frow, 1.0, 0.0).astype(BF16), x[...])
    sums[...] = jnp.zeros_like(sums)
    sums[tm : 2 * tm, :] = x_sum[:tm]
    trow = lax.broadcasted_iota(jnp.int32, (fp, LANES), 0)
    tlane = lax.broadcasted_iota(jnp.int32, (fp, LANES), 1)
    tile[...] = jnp.where((trow == t) & (tlane == both + codes[0, 0]), 1.0, 0.0).astype(F32)
    x_part = reduce_rows(x_sum, wps, both)

    pair = 2 * rows
    columns = 512

    def project(p, first, last):
        base = pl.multiple_of(ring_chip((p + 2 * chips) % chips, chips) * pair, pair)

        for n in range(3 * width // columns):
            at = slice(n * columns, (n + 1) * columns)
            got = dot(normed[:, pl.ds(base, pair)], wq[pl.ds(base, pair), at])
            if not first:
                got = got + acc[:, at]
            if last:
                qkv[:, at] = got.astype(BF16)
            else:
                acc[:, at] = got

    def wait_sib(d, s, h):
        sib_copy(d, s, h).wait_recv()

    by_chip = pair % LANES == 0
    for h in range(2):
        wait_sib(0, 0, h)
    if by_chip:
        project(spot, True, chips == 1)
    def pass_maps():
        for k in range(1, chips):
            remote(mt_all.at[i], mt_all.at[i], ("far", k), i, t).wait_recv()
            go(map_copy(k))

    if sharing:
        for d in range(2):
            twin_copy(d).wait_recv()
            go(quarter_sib(d, 1))
        pass_maps()
        for d in range(2):
            for n in range(2):
                main_sib(d, 1, n).wait_recv()
                quarter_sib(d, n).wait_recv()
            if by_chip:
                project(spot - dirs[d], False, False)
            if d == 0:
                for e in range(2):
                    take_main(e, 1, 0)
    else:
        for s in range(half_ring):
            for d in range(2):
                for n, h in enumerate(halves(d, s)):
                    if not (half_ring > 1 and s == 0 and n == 0):
                        take(d, s, h)
            if s < half_ring - 1:
                for d in range(2):
                    for h in halves(d, s):
                        wait_sib(d, s + 1, h)
                    if by_chip:
                        project(spot - dirs[d] * (s + 1), False, False)

    if not sharing:
        pass_maps()
    for k in range(chips):
        map_copy(k).wait_recv()
    mts[...] = three_parts(jnp.concatenate([mt_all[n] for n in range(dp)], axis=1))

    if sharing:
        for d in range(2):
            take_main(d, 1, 1)
        for d in range(2):
            for n in range(2):
                main_sib(d, 2, n).wait_recv()
    else:
        for d in range(2):
            for h in halves(d, half_ring - 1):
                wait_sib(d, half_ring, h)
    if by_chip:
        project(spot + half_ring, False, True)
    else:
        def whole_body(n, carry):
            at = pl.ds(pl.multiple_of(n * columns, columns), columns)
            qkv[:, at] = dot(normed[...], wq[:, at]).astype(BF16)
            return carry

        lax.fori_loop(0, 3 * width // columns, whole_body, 0)

    scale_q = HEAD_DIM ** (-0.5)

    def frame(f):
        return slice(f * mine, (f + 1) * mine)

    scores = [None] * tm
    for f in range(tm):
        q = qkv[frame(f), 0:width]
        products = jnp.concatenate([q] * (f + 1), axis=0) * qkv[0 : (f + 1) * mine, width : 2 * width]
        r = dot(products, place[f * width : (f + 1) * width, :])
        for g in range(f + 1):
            scores[g] = r[frame(g)] if scores[g] is None else scores[g] + r[frame(g)]
    lane_frame = lax.broadcasted_iota(jnp.int32, (mine, lanes), 1) // heads
    scores = [jnp.where(lane_frame >= g, s * scale_q, -1e30) for g, s in enumerate(scores)]
    top = functools.reduce(jnp.maximum, scores)
    raised = [jnp.exp(s - top) for s in scores]
    whole = functools.reduce(jnp.add, raised)
    for g in range(tm):
        w = raised[g] / whole
        w_full[frame(g), :] = w
        w_low[frame(g), :] = w.astype(BF16)
    mixed = dot(w_low[...], qkv[:, 2 * width :], 0, 0) * lift[...].astype(F32)
    sums[0:tm, :] = jnp.sum(mixed.reshape(tm, heads, width), axis=1)

    tile[:, :both] = (reduce_rows(sums[0:fp, :], mts, both) + x_part) * (1.0 / patches)
    for r in range(1, tm):
        go(remote(tile, tile_all.at[t], ("tile", r), i, (t + r) % tm))
    for r in range(1, tm):
        go(remote(sums, sums_all.at[t], ("sum", r), i, (t + r) % tm))
    tile_all[t] = tile[...]
    sums_all[t] = sums[...]
    for r in range(1, tm):
        remote(tile, tile_all.at[t], ("tile", r), i, t).wait_recv()

    tot = tile_all[0]
    for r in range(1, tm):
        tot = tot + tile_all[r]
    lrow = lax.broadcasted_iota(jnp.int32, (fp, latent), 0)
    following = jnp.where(lrow < tm - 1, pltpu.roll(tot, fp - 1, 0)[:, latent:both], 0.0)
    onehot = tot[:, both : both + n_codes]
    quantized = onehot[:, 0:1] * codebook[0:1, :]
    for n in range(1, n_codes):
        quantized = quantized + onehot[:, n : n + 1] * codebook[n : n + 1, :]
    d_action = jnp.where(lrow < tm, (2.0 * BETA) * (tot[:, :latent] + following - quantized), 0.0)
    earlier = jnp.where((lrow > 0) & (lrow < tm), pltpu.roll(d_action, 1, 0), 0.0)
    d_pair = jnp.concatenate([d_action, earlier], axis=1)
    d_att[...] = expand_rows(d_pair, mts).astype(BF16).astype(F32)
    d_rows[...] = expand_rows(d_pair, wps)

    for f in range(tm):
        at = slice(f * heads, (f + 1) * heads)
        d_big[at, :] = (lift[at, :].astype(F32) * d_att[f : f + 1, :]).astype(BF16)
    d_w = dot(qkv[:, 2 * width :], d_big[...], 1, 1).astype(BF16).astype(F32)
    wd = [w_full[frame(g), :] * d_w[frame(g)] for g in range(tm)]
    mean = functools.reduce(jnp.add, wd)
    for g in range(tm):
        d_s[frame(g), :] = ((wd[g] - w_full[frame(g), :] * mean) * scale_q).astype(BF16).astype(F32)

    wide = 256

    def backward(n):
        def own(f):
            return slice(f * mine + n * sub, f * mine + (n + 1) * sub)

        def at(f):
            return slice(n * part_rows + f * sub, n * part_rows + (f + 1) * sub)

        lane_f = lax.broadcasted_iota(jnp.int32, (sub, lanes), 1) // heads
        picked = [
            jnp.concatenate([jnp.where(lane_f == f, d_s[own(g), :], 0.0) for g in range(f + 1)], axis=0).astype(BF16)
            for f in range(tm)
        ]
        for c in range(0, width, wide):
            k = [qkv[own(g), width + c : width + c + wide].astype(F32) for g in range(tm)]
            dk = [None] * tm
            for f in range(tm):
                q = qkv[own(f), c : c + wide].astype(F32)
                spread = dot(picked[f], lift[:, c : c + wide])
                dq = None
                for g in range(f + 1):
                    s = spread[g * sub : (g + 1) * sub]
                    dq = s * k[g] if dq is None else dq + s * k[g]
                    dk[g] = s * q if dk[g] is None else dk[g] + s * q
                dqkv[at(f), c : c + wide] = dq.astype(BF16)
            for g in range(tm):
                dqkv[at(g), width + c : width + c + wide] = dk[g].astype(BF16)
        low = jnp.concatenate([w_low[own(g), :] for g in range(tm)], axis=0)
        group = slice(n * part_rows, (n + 1) * part_rows)
        dqkv[group, 2 * width :] = dot(low, d_big[...]).astype(BF16)
        for c in range(0, width, 512):
            dn[:, c : c + 512] = dot(dqkv[group, :], wq[c : c + 512, :], 1, 1).astype(BF16)
        for f in range(tm):
            xf = x[own(f), :].astype(F32)
            scale = scales[own(f), 0:1]
            u = dn[f * sub : (f + 1) * sub, :].astype(F32) * gain_row
            inner = jnp.mean(xf * u, axis=-1, keepdims=True)
            dx = u * scale - xf * (scale * scale * scale * inner)
            done[at(f), :] = (d_rows[f : f + 1, :] + dx).astype(BF16)

    def done_copy(n, r, other):
        return remote(
            done.at[pl.ds(pl.multiple_of(n * part_rows + other * sub, sub), sub)],
            out.at[pl.ds(pl.multiple_of(t * mine + n * sub, sub), sub)], ("done", n, r), i, other,
        )

    def give(n):
        for r in sorted(range(1, tm), key=lambda r: -min(r, tm - r)):
            go(done_copy(n, r, (t + r) % tm))
        out[pl.ds(pl.multiple_of(t * mine + n * sub, sub), sub), :] = done[
            pl.ds(pl.multiple_of(n * part_rows + t * sub, sub), sub), :
        ]

    def share():
        for r in range(1, tm):
            remote(sums, sums_all.at[t], ("sum", r), i, t).wait_recv()
        s = sums_all[0]
        for r in range(1, tm):
            s = s + sums_all[r]
        s = s * (1.0 / patches)
        for n in range(dp):
            msg[n] = jnp.zeros_like(msg[n])
            msg[n, 0, :, 0:rows] = s[:, n * rows : (n + 1) * rows]
            msg[n, 1, 0:tm, 0:both] = d_pair[:tm]
            msg[n, 1, 0:tm, both : both + n_codes] = onehot[:tm]
        for r in range(1, dp):
            other = (i + r) % dp
            go(remote(msg.at[other], msg_all.at[i], ("msg", r), other, t))
        msg_all[i] = msg[i]

    for n in range(groups):
        backward(n)
        give(n)
        if n == 0:
            share()

    for r in range(1, dp):
        remote(msg.at[i], msg_all.at[i], ("msg", r), i, t).wait_recv()
    turn = rows % LANES != 0

    def turned(v):
        return v.T if turn else v

    every = dp * sr
    kept = dp * tm
    slices = msg_all[:, 0].reshape(every, LANES)
    krow = lax.broadcasted_iota(jnp.int32, (kept, every), 0)
    kcol = lax.broadcasted_iota(jnp.int32, (kept, every), 1)
    source = (krow // tm) * sr + krow % tm
    pick = jnp.where(kcol == source, 1.0, 0.0).astype(F32)
    mixed_rows = dot(pick, slices, precision=HIGH)
    mapped = dot_split(mixed_rows[:, :rows], wo[...])
    for n in range(dp):
        part[n] = turned(mapped[:, n * rows : (n + 1) * rows])
    for r in range(1, dp):
        other = (i + r) % dp
        go(remote(part.at[other], part_all.at[i], ("part", r), other, t))
    plain_rows = dot(jnp.where(kcol == source + tm, 1.0, 0.0).astype(F32), slices, precision=HIGH)
    part_all[i] = part[i] + turned(plain_rows[:, :rows])
    marks = msg_all[:, 1].reshape(every, LANES)
    table = dot(marks, marks, 0, 0, precision=HIGH)[both : both + n_codes]
    count = jnp.sum(table[:, both : both + n_codes], axis=1, keepdims=True)
    d_pairs = dot(pick, marks, precision=HIGH)
    step_out[...] = table[:, :latent] * (-1.0 / BETA) / count

    for r in range(1, dp):
        remote(part.at[i], part_all.at[i], ("part", r), i, t).wait_recv()
    final = part_all[0]
    for n in range(1, dp):
        final = final + part_all[n]
    final_all[i] = final
    for r in range(1, dp):
        go(remote(final_all.at[i], final_all.at[i], ("final", r), (i + r) % dp, t))
    for r in range(1, dp):
        remote(final_all.at[i], final_all.at[i], ("final", r), i, t).wait_recv()
    pooled = jnp.concatenate([final_all[n] for n in range(dp)], axis=0 if turn else 1)
    grads = dot(d_pairs, pooled, 0, 1 if turn else 0, precision=HIGH)
    for m in range(2):
        pair_out[m] = grads[m * latent : (m + 1) * latent]

    for n in range(groups):
        for r in range(1, tm):
            done_copy(n, r, t).wait_recv()
    for copy in started:
        copy.wait_send()
    assert len(tags) <= send.shape[0]


def write_out(grad, pair, step, grad_out, pair_out, step_out, sem):
    copies = [
        pltpu.make_async_copy(src, dst, sem.at[n])
        for n, (src, dst) in enumerate(((grad, grad_out), (pair, pair_out), (step, step_out)))
    ]
    for copy in copies:
        copy.start()
    for copy in copies:
        copy.wait()


def local(dp, tm, tokens, gain, w_qkv, w_out, w_pair, codebook, codes):
    patches, width = tokens.shape[2:]
    rows = w_qkv.shape[0]
    latent, n_codes = w_pair.shape[2], codebook.shape[0]
    both = 2 * latent
    fp = -(-tm // 8) * 8
    sr = -(-2 * tm // 8) * 8
    lanes = tm * (width // HEAD_DIM)
    groups = 2 if patches // tm % 32 == 0 else 1
    part_rows = patches // groups
    assert rows <= LANES and 2 * both <= LANES and both + n_codes <= LANES
    slab = (rows, dp * tm) if rows % LANES else (dp * tm, rows)
    tags = (tm - 1) * (3 + groups) + 3 * (dp - 1) + 5 * dp + 16
    vmem = pl.BlockSpec(memory_space=pltpu.VMEM)
    hbm = pl.BlockSpec(memory_space=pltpu.HBM)
    grad, pair, step = pl.pallas_call(
        functools.partial(kernel, (dp, tm, rows, patches, width, latent, n_codes, groups)),
        out_shape=(
            pltpu.VMEM((patches, width), BF16),
            pltpu.VMEM((2, latent, width), F32),
            pltpu.VMEM((n_codes, latent), F32),
        ),
        in_specs=[hbm] * 7,
        out_specs=(vmem, vmem, vmem),
        scratch_shapes=[
            pltpu.VMEM((dp * rows, 3 * width), BF16),
            pltpu.VMEM((rows, width), BF16),
            pltpu.VMEM((both, width), F32),
            pltpu.VMEM((width,), BF16),
            pltpu.VMEM((n_codes, latent), F32),
            pltpu.SMEM((1, 1), jnp.int32),
            pltpu.VMEM((patches, width), BF16),
            pltpu.VMEM((patches, width), BF16),
            pltpu.VMEM((patches, LANES), F32),
            pltpu.VMEM((patches if 2 * rows % LANES == 0 else 8, 3 * width), F32),
            pltpu.VMEM((patches, 3 * width), BF16),
            pltpu.VMEM((tm * width, lanes), BF16),
            pltpu.VMEM((lanes, width), BF16),
            pltpu.VMEM((patches, lanes), F32),
            pltpu.VMEM((patches, lanes), BF16),
            pltpu.VMEM((lanes, width), BF16),
            pltpu.VMEM((patches, lanes), F32),
            pltpu.VMEM((patches, 3 * width), BF16),
            pltpu.VMEM((part_rows, width), BF16),
            pltpu.VMEM((patches, width), BF16),
            pltpu.VMEM((fp, width), F32),
            pltpu.VMEM((fp, width), F32),
            pltpu.VMEM((3 * both, width), BF16),
            pltpu.VMEM((3 * both, width), BF16),
            pltpu.VMEM((dp, both, rows), F32),
            pltpu.VMEM((fp, LANES), F32),
            pltpu.VMEM((tm, fp, LANES), F32),
            pltpu.VMEM((sr, width), F32),
            pltpu.VMEM((tm, sr, width), F32),
            pltpu.VMEM((dp, 2, sr, LANES), F32),
            pltpu.VMEM((dp, 2, sr, LANES), F32),
            pltpu.VMEM((dp, *slab), F32),
            pltpu.VMEM((dp, *slab), F32),
            pltpu.VMEM((dp, *slab), F32),
            pltpu.SemaphoreType.DMA((tags,)),
            pltpu.SemaphoreType.DMA((tags,)),
            pltpu.SemaphoreType.DMA((7,)),
        ],
        compiler_params=pltpu.CompilerParams(
            collective_id=0, has_side_effects=True, vmem_limit_bytes=60000 * 1024
        ),
    )(
        tokens.reshape(patches, width), gain, w_qkv, w_out, w_pair.swapaxes(1, 2).reshape(both, width), codebook,
        codes.reshape(1, 1),
    )
    made = (grad, pair, step)
    grad, pair, step = pl.pallas_call(
        write_out,
        out_shape=tuple(jax.ShapeDtypeStruct(v.shape, v.dtype) for v in made),
        in_specs=[vmem] * 3,
        out_specs=(hbm, hbm, hbm),
        scratch_shapes=[pltpu.SemaphoreType.DMA((3,))],
        compiler_params=pltpu.CompilerParams(vmem_limit_bytes=4096 * 1024),
    )(*made)
    return grad.reshape(tokens.shape), pair.swapaxes(1, 2), step


def solution(mesh):
    placed = (
        P("dp", "tm", None, None),
        P(),
        P("dp", None),
        P("dp", None),
        P(),
        P(),
        P("dp", "tm", None),
    )
    return jax.shard_map(
        functools.partial(local, mesh.shape["dp"], mesh.shape["tm"]),
        mesh=mesh,
        in_specs=placed,
        out_specs=(P("dp", "tm", None, None), P(), P()),
        check_vma=False,
    )
```

```python
import functools

import jax
import jax.numpy as jnp
from jax import lax
from jax.experimental import pallas as pl
from jax.experimental.pallas import tpu as pltpu
from jax.sharding import PartitionSpec as P

HEAD_DIM = 64
EPS = 1e-06
BETA = 0.25
LANES = 128
F32 = jnp.float32
BF16 = jnp.bfloat16
HIGH = lax.Precision.HIGHEST


def dot(a, b, ca=1, cb=0, precision=None):
    return lax.dot_general(
        a, b, (((ca,), (cb,)), ((), ())), precision=precision, preferred_element_type=F32
    )


def dot_split(a, b, cb=0):
    high = a.astype(BF16)
    rest = a - high.astype(F32)
    mid = rest.astype(BF16)
    low = (rest - mid.astype(F32)).astype(BF16)
    n = a.shape[0]
    terms = jnp.concatenate([high.astype(F32), mid.astype(F32), low.astype(F32)], axis=0)
    out = dot(terms.astype(BF16), b, 1, cb)
    return out[:n] + out[n : 2 * n] + out[2 * n :]


def bits_of(n):
    return max(n.bit_length() - 1, 0)


def ring_place(chip, n):
    b = [(chip // 2**k) % 2 for k in range(bits_of(n))]
    return sum(((sum(b[k:]) % 2) * 2**k for k in range(len(b))), 0)


def ring_chip(place, n):
    count = bits_of(n)
    b = [(place // 2**k) % 2 for k in range(count)] + [0]
    return sum((((b[k] + b[k + 1]) % 2) * 2**k for k in range(count)), 0)


def split2(a):
    high = a.astype(BF16).astype(F32)
    return high, a - high


def reduce_rows(v, parts, n):
    high, mid = split2(v)
    r = dot(jnp.concatenate([high, mid], axis=0).astype(BF16), parts[0 : 2 * n, :], 1, 1)
    r = r[: v.shape[0]] + r[v.shape[0] :]
    return r[:, :n] + r[:, n : 2 * n]


def expand_rows(b, parts):
    high, mid = split2(b)
    return dot(jnp.concatenate([high, high, mid], axis=1).astype(BF16), parts[...])


def three_parts(value):
    high, mid = split2(value)
    return jnp.concatenate([high, mid, high], axis=0).astype(BF16)


def kernel(
    cfg, tokens, gain_in, wq_own, wo_in, wp_in, codebook_in, codes_in,
    out, pair_out, step_out,
    wq, wo, wp, gain, codebook, codes, x, normed, scales, acc, qkv, place, lift,
    raw, w_full, w_low, d_big, d_s, slope, dqkv, done, d_rows, d_att,
    wps, mts, mt_all, tile, tile_all, sums, sums_all, msg, msg_all, part, part_all, final_all,
    send, recv, local_sem,
):
    dp, tm, rows, patches, width, latent, n_codes, pieces = cfg
    mine = patches // tm
    total = tm * mine
    sub = 32 if mine % 32 == 0 else mine
    wide = width // pieces
    fp, sr = tile.shape[0], sums.shape[0]
    heads = width // HEAD_DIM
    lanes = tm * heads
    both = 2 * latent
    chips = dp // 2
    half_ring = chips // 2
    i = lax.axis_index("dp")
    t = lax.axis_index("tm")
    core = i % 2
    spot = ring_place(i // 2, chips)

    def device_at(p, c):
        return ring_chip((p + 2 * chips) % chips, chips) * 2 + c

    barrier = pltpu.get_barrier_semaphore()
    for r in range(1, tm):
        pl.semaphore_signal(barrier, inc=1, device_id={"dp": i, "tm": (t + r) % tm})
    for r in range(1, dp):
        pl.semaphore_signal(barrier, inc=1, device_id={"dp": (i + r) % dp, "tm": t})

    def frame_rows(f):
        return pl.ds(pl.multiple_of(f * mine, mine), mine)

    half = rows // 2
    dirs = (1, -1)
    quarter = half // 2
    sharing = half_ring == 2 and quarter % 16 == 0 and tm % 2 == 0
    odd = t % 2
    twin = t + 1 - 2 * odd

    def own_at(at, n):
        return wq_own.at[pl.ds(pl.multiple_of(at, n), n)], wq.at[pl.ds(pl.multiple_of(i * rows + at, n), n)]

    if sharing:
        loads = [
            own_at(h * half + which * quarter, quarter) for which in (odd, 1 - odd) for h in (1, 0)
        ]
    else:
        loads = [own_at(0, rows)]
    loads = [
        pltpu.make_async_copy(src, dst, local_sem.at[6 + n]) for n, (src, dst) in enumerate(loads)
    ]
    here = [
        pltpu.make_async_copy(src, dst, local_sem.at[n])
        for n, (src, dst) in enumerate((
            (wp_in, wp),
            (wo_in, wo),
            (tokens.at[frame_rows(t)], x.at[frame_rows(t)]),
            (gain_in, gain),
            (codebook_in, codebook),
            (codes_in, codes),
        ))
    ]
    for copy in loads + here:
        copy.start()

    col_head = lax.broadcasted_iota(jnp.int32, (width, lanes), 0) // HEAD_DIM
    lane_id = lax.broadcasted_iota(jnp.int32, (width, lanes), 1)
    for f in range(tm):
        place[f * width : (f + 1) * width, :] = jnp.where(lane_id == f * heads + col_head, 1.0, 0.0).astype(BF16)
    row_head = lax.broadcasted_iota(jnp.int32, (lanes, width), 0) % heads
    lift_col = lax.broadcasted_iota(jnp.int32, (lanes, width), 1) // HEAD_DIM
    lift[...] = jnp.where(row_head == lift_col, 1.0, 0.0).astype(BF16)

    tags = {}

    def tag(*key):
        return tags.setdefault(key, len(tags))

    started = []

    def remote(src, dst, key, dpi, tmi):
        k = tag(*key)
        return pltpu.make_async_remote_copy(
            src_ref=src, dst_ref=dst, send_sem=send.at[k], recv_sem=recv.at[k],
            device_id={"dp": dpi, "tm": tmi},
        )

    def go(copy):
        copy.start()
        started.append(copy)

    def go_all(key, copies, landing):
        for copy in copies:
            copy.start()
        started.append(remote(landing, landing, key, i, t))

    def landed(key, landing):
        remote(landing, landing, key, i, t).wait_recv()

    def settle(copies):
        for copy in copies:
            copy.wait_send()

    def piece(origin, h):
        return wq.at[pl.ds(pl.multiple_of(origin * rows + h * half, half), half)]

    def main_half(d):
        return 0 if dirs[d] == 1 else 1

    def halves(d, s):
        first = main_half(d)
        return (first, 1 - first) if s < half_ring - 1 else (first,)

    def quarter_of(origin, h, which):
        at = origin * rows + h * half + which * quarter
        return wq.at[pl.ds(pl.multiple_of(at, quarter), quarter)]

    def ring_copy(d, s, h):
        ref = piece(device_at(spot - dirs[d] * s, core), h)
        return remote(ref, ref, ("ring", d, s, h), device_at(spot + dirs[d], core), t)

    def sib_copy(d, s, h):
        ref = piece(device_at(spot - dirs[d] * s, core), h)
        return remote(ref, ref, ("sib", d, s, h), device_at(spot, 1 - core), t)

    def take(d, s, h):
        ring_copy(d, s, h).wait_recv()
        if s + 1 < half_ring and h in halves(d, s + 1):
            go(ring_copy(d, s + 1, h))
        go(sib_copy(d, s + 1, h))

    def shared_copy(d):
        ref = quarter_of(i, 1 - main_half(d), odd)
        return remote(ref, ref, ("shared", d), device_at(spot + dirs[d], core), t)

    def twin_copy(d):
        at = quarter_of(device_at(spot - dirs[d], core), 1 - main_half(d), odd)
        return remote(at, at, ("twin", d), i, twin)

    def quarter_sib(d, n):
        which = odd if n == 0 else 1 - odd
        at = quarter_of(device_at(spot - dirs[d], core), 1 - main_half(d), which)
        return remote(at, at, ("quarter", d, n), device_at(spot, 1 - core), t)

    def main_copy(d, s, n):
        ref = quarter_of(device_at(spot - dirs[d] * s, core), main_half(d), n)
        return remote(ref, ref, ("main", d, s, n), device_at(spot + dirs[d], core), t)

    def main_sib(d, s, n):
        ref = quarter_of(device_at(spot - dirs[d] * s, core), main_half(d), n)
        return remote(ref, ref, ("mainsib", d, s, n), device_at(spot, 1 - core), t)

    def take_main(d, s, n):
        main_copy(d, s, n).wait_recv()
        if s == 0:
            go(main_copy(d, 1, n))
        go(main_sib(d, s + 1, n))

    map_rows = both // tm if both // tm % 8 == 0 else both

    def map_part(origin):
        if map_rows == both:
            return mt_all.at[origin]
        return mt_all.at[origin, pl.ds(pl.multiple_of(t * map_rows, map_rows), map_rows)]

    def map_copy(k):
        at = mt_all.at[device_at(spot - k, core)]
        return remote(at, at, ("map",), device_at(spot, 1 - core), t)

    def map_far(k):
        at = map_part(i)
        return remote(at, at, ("far", k), device_at(spot + k, core), t)

    def map_near(k, r):
        at = map_part(device_at(spot - k, core))
        return remote(at, at, ("near", k), i, (t + r) % tm)

    near_rows = mt_all.at[0, 0 : (tm - 1) * map_rows] if map_rows != both else None

    def pass_far():
        for k in range(1, chips):
            map_far(k).wait_recv()
            if map_rows != both:
                go_all(("near", k), [map_near(k, r) for r in range(1, tm)], near_rows)

    def pass_near():
        if map_rows != both:
            for k in range(1, chips):
                landed(("near", k), near_rows)
        go_all(("map",), [map_copy(k) for k in range(chips)], mt_all.at[0:chips])

    loads[0].wait()
    pl.semaphore_wait(barrier, tm + dp - 2)
    if sharing:
        go(shared_copy(0))
        loads[1].wait()
        go(shared_copy(1))
        for copy in loads[2:]:
            copy.wait()
        for n in range(2):
            for d in range(2):
                go(main_copy(d, 0, n))
    else:
        for n in range(2):
            for d in range(2):
                if n < len(halves(d, 0)):
                    go(ring_copy(d, 0, halves(d, 0)[n]))
    others = sorted(range(1, tm), key=lambda r: -min(r, tm - r))
    go_all(("tok",), [
        remote(tokens.at[frame_rows((t + r) % tm)], x.at[frame_rows(t)], ("tok",), i, (t + r) % tm) for r in others
    ], x.at[0 : (tm - 1) * mine])
    for h in range(2):
        go(sib_copy(0, 0, h))

    for copy in here:
        copy.wait()
    mt_all[i] = dot_split(wp[...], wo[...], 1)
    for k in range(1, chips):
        go(map_far(k))
    wps[...] = three_parts(wp[...])

    if sharing:
        for d in range(2):
            shared_copy(d).wait_recv()
            go(twin_copy(d))
            go(quarter_sib(d, 0))
        for n in range(2):
            for d in range(2):
                take_main(d, 0, n)
        pass_far()
    elif half_ring > 1:
        for d in range(2):
            take(d, 0, main_half(d))

    landed(("tok",), x.at[0 : (tm - 1) * mine])

    block = 32
    gain_row = gain[...].astype(F32).reshape(1, width)

    def norm_step(b, carry):
        at = pl.ds(pl.multiple_of(b * block, block), block)
        xf = x[at, :].astype(F32)
        scale = lax.rsqrt(jnp.mean(xf * xf, axis=-1, keepdims=True) + EPS)
        scales[at, :] = jnp.broadcast_to(scale, (block, LANES))
        normed[at, :] = (xf * scale * gain_row).astype(BF16)
        return carry

    lax.fori_loop(0, total // block, norm_step, 0)

    frow = lax.broadcasted_iota(jnp.int32, (fp, total), 0)
    fcol = lax.broadcasted_iota(jnp.int32, (fp, total), 1)
    x_sum = dot(jnp.where(fcol // mine == frow, 1.0, 0.0).astype(BF16), x[...])
    sums[...] = jnp.zeros_like(sums)
    sums[tm : 2 * tm, :] = x_sum[:tm]
    trow = lax.broadcasted_iota(jnp.int32, (fp, LANES), 0)
    tlane = lax.broadcasted_iota(jnp.int32, (fp, LANES), 1)
    tile[...] = jnp.where((trow == t) & (tlane == both + codes[0, 0, 0]), 1.0, 0.0).astype(F32)
    x_part = reduce_rows(x_sum, wps, both)

    pair = 2 * rows
    columns = 512

    def project(p, first, last):
        base = pl.multiple_of(ring_chip((p + 2 * chips) % chips, chips) * pair, pair)

        for n in range(3 * width // columns):
            at = slice(n * columns, (n + 1) * columns)
            got = dot(normed[:, pl.ds(base, pair)], wq[pl.ds(base, pair), at])
            if not first:
                got = got + acc[:, at]
            if last:
                qkv[:, at] = got.astype(BF16)
            else:
                acc[:, at] = got

    def wait_sib(d, s, h):
        sib_copy(d, s, h).wait_recv()

    by_chip = pair % LANES == 0
    for h in range(2):
        wait_sib(0, 0, h)
    if by_chip:
        project(spot, True, chips == 1)
    if sharing:
        for d in range(2):
            twin_copy(d).wait_recv()
            go(quarter_sib(d, 1))
        pass_near()
        for d in range(2):
            for n in range(2):
                main_sib(d, 1, n).wait_recv()
                quarter_sib(d, n).wait_recv()
            if by_chip:
                project(spot - dirs[d], False, False)
            if d == 0:
                for e in range(2):
                    take_main(e, 1, 0)
    else:
        for s in range(half_ring):
            for d in range(2):
                for n, h in enumerate(halves(d, s)):
                    if not (half_ring > 1 and s == 0 and n == 0):
                        take(d, s, h)
            if s < half_ring - 1:
                for d in range(2):
                    for h in halves(d, s):
                        wait_sib(d, s + 1, h)
                    if by_chip:
                        project(spot - dirs[d] * (s + 1), False, False)

    if not sharing:
        pass_far()
        pass_near()
    landed(("map",), mt_all.at[0:chips])
    mts[...] = three_parts(jnp.concatenate([mt_all[n] for n in range(dp)], axis=1))

    if sharing:
        for d in range(2):
            take_main(d, 1, 1)
        for d in range(2):
            for n in range(2):
                main_sib(d, 2, n).wait_recv()
    else:
        for d in range(2):
            for h in halves(d, half_ring - 1):
                wait_sib(d, half_ring, h)
    if by_chip:
        project(spot + half_ring, False, True)
    else:
        def whole_body(n, carry):
            at = pl.ds(pl.multiple_of(n * columns, columns), columns)
            qkv[:, at] = dot(normed[...], wq[:, at]).astype(BF16)
            return carry

        lax.fori_loop(0, 3 * width // columns, whole_body, 0)

    scale_q = HEAD_DIM ** (-0.5)

    def frame(f):
        return slice(f * mine, (f + 1) * mine)

    scores = [None] * tm
    for f in range(tm):
        q = qkv[frame(f), 0:width]
        products = jnp.concatenate([q] * (f + 1), axis=0) * qkv[0 : (f + 1) * mine, width : 2 * width]
        r = dot(products, place[f * width : (f + 1) * width, :])
        for g in range(f + 1):
            scores[g] = r[frame(g)] if scores[g] is None else scores[g] + r[frame(g)]
    lane_frame = lax.broadcasted_iota(jnp.int32, (mine, lanes), 1) // heads
    for g in range(tm):
        raw[frame(g), :] = scores[g]
    scores = [jnp.where(lane_frame >= g, s * scale_q, -1e30) for g, s in enumerate(scores)]
    top = functools.reduce(jnp.maximum, scores)
    raised = [jnp.exp(s - top) for s in scores]
    whole = functools.reduce(jnp.add, raised)
    for g in range(tm):
        w = raised[g] / whole
        w_full[frame(g), :] = w
        w_low[frame(g), :] = w.astype(BF16)
    mixed = dot(w_low[...], qkv[:, 2 * width :], 0, 0) * lift[...].astype(F32)
    sums[0:tm, :] = jnp.sum(mixed.reshape(tm, heads, width), axis=1)

    tile[:, :both] = (reduce_rows(sums[0:fp, :], mts, both) + x_part) * (1.0 / patches)
    before = list(started)
    started.clear()
    go_all(("tile",), [
        remote(tile, tile_all.at[t], ("tile",), i, (t + r) % tm) for r in others
    ], tile_all.at[0 : tm - 1])
    go_all(("sum",), [
        remote(sums, sums_all.at[t], ("sum",), i, (t + r) % tm) for r in others
    ], sums_all.at[0 : tm - 1])
    tile_all[t] = tile[...]
    sums_all[t] = sums[...]
    settle(before)
    landed(("tile",), tile_all.at[0 : tm - 1])

    tot = tile_all[0]
    for r in range(1, tm):
        tot = tot + tile_all[r]
    lrow = lax.broadcasted_iota(jnp.int32, (fp, latent), 0)
    following = jnp.where(lrow < tm - 1, pltpu.roll(tot, fp - 1, 0)[:, latent:both], 0.0)
    onehot = tot[:, both : both + n_codes]
    quantized = onehot[:, 0:1] * codebook[0:1, :]
    for n in range(1, n_codes):
        quantized = quantized + onehot[:, n : n + 1] * codebook[n : n + 1, :]
    d_action = jnp.where(lrow < tm, (2.0 * BETA) * (tot[:, :latent] + following - quantized), 0.0)
    earlier = jnp.where((lrow > 0) & (lrow < tm), pltpu.roll(d_action, 1, 0), 0.0)
    d_pair = jnp.concatenate([d_action, earlier], axis=1)
    d_att[...] = expand_rows(d_pair, mts).astype(BF16).astype(F32)
    d_rows[...] = expand_rows(d_pair, wps)

    for f in range(tm):
        at = slice(f * heads, (f + 1) * heads)
        d_big[at, :] = (lift[at, :].astype(F32) * d_att[f : f + 1, :]).astype(BF16)
    d_w = dot(qkv[:, 2 * width :], d_big[...], 1, 1).astype(BF16).astype(F32)
    wd = [w_full[frame(g), :] * d_w[frame(g)] for g in range(tm)]
    mean = functools.reduce(jnp.add, wd)
    through = []
    for g in range(tm):
        d = ((wd[g] - w_full[frame(g), :] * mean) * scale_q).astype(BF16).astype(F32)
        d_s[frame(g), :] = d
        through.append(d * raw[frame(g), :])
    through_all = functools.reduce(jnp.add, through)
    for g in range(tm):
        value = wd[g] + through[g] + jnp.where(lane_frame == g, through_all, 0.0)
        scale = scales[frame(g), 0:1]
        value = jnp.sum(value, axis=-1, keepdims=True) * (1.0 / width) * scale * scale
        slope[frame(g), :] = jnp.broadcast_to(value, (mine, LANES))

    lane_f = lax.broadcasted_iota(jnp.int32, (sub, lanes), 1) // heads
    block_c = 256
    for n in range(mine // sub):
        def own(f):
            return slice(f * mine + n * sub, f * mine + (n + 1) * sub)

        picked = [
            jnp.concatenate([jnp.where(lane_f == f, d_s[own(g), :], 0.0) for g in range(f + 1)], axis=0).astype(BF16)
            for f in range(tm)
        ]
        for c in range(0, width, block_c):
            k = [qkv[own(g), width + c : width + c + block_c].astype(F32) for g in range(tm)]
            dk = [None] * tm
            for f in range(tm):
                q = qkv[own(f), c : c + block_c].astype(F32)
                spread = dot(picked[f], lift[:, c : c + block_c])
                dq = None
                for g in range(f + 1):
                    v = spread[g * sub : (g + 1) * sub]
                    dq = v * k[g] if dq is None else dq + v * k[g]
                    dk[g] = v * q if dk[g] is None else dk[g] + v * q
                dqkv[own(f), c : c + block_c] = dq.astype(BF16)
            for g in range(tm):
                dqkv[own(g), width + c : width + c + block_c] = dk[g].astype(BF16)
    dqkv[:, 2 * width :] = dot(w_low[...], d_big[...]).astype(BF16)

    def done_copy(n, r, other):
        at = pl.ds(n * wide, wide)
        return remote(done.at[frame_rows(other), at], out.at[frame_rows(t), at], ("done",), i, other)

    def give(n):
        at = slice(n * wide, (n + 1) * wide)
        dn = dot(dqkv[...], wq[at, :], 1, 1).astype(BF16).astype(F32)
        for f in range(tm):
            u = dn[frame(f)] * gain_row[:, at]
            dx = u * scales[frame(f), 0:1] - x[frame(f), at].astype(F32) * slope[frame(f), 0:1]
            done[frame(f), at] = (d_rows[f : f + 1, at] + dx).astype(BF16)
        for r in others:
            done_copy(n, r, (t + r) % tm).start()
        out[frame_rows(t), at] = done[frame_rows(t), at]

    def share():
        landed(("sum",), sums_all.at[0 : tm - 1])
        s = sums_all[0]
        for r in range(1, tm):
            s = s + sums_all[r]
        s = s * (1.0 / patches)
        for n in range(dp):
            msg[n] = jnp.zeros_like(msg[n])
            msg[n, 0, :, 0:rows] = s[:, n * rows : (n + 1) * rows]
            msg[n, 1, 0:tm, 0:both] = d_pair[:tm]
            msg[n, 1, 0:tm, both : both + n_codes] = onehot[:tm]
        go_all(("msg",), [
            remote(msg.at[(i + r) % dp], msg_all.at[i], ("msg",), (i + r) % dp, t) for r in range(1, dp)
        ], msg_all.at[0 : dp - 1])
        msg_all[i] = msg[i]

    for n in range(pieces):
        give(n)
        if n == 0:
            share()

    landed(("msg",), msg_all.at[0 : dp - 1])
    turn = rows % LANES != 0

    def turned(v):
        return v.T if turn else v

    every = dp * sr
    kept = dp * tm
    slices = msg_all[:, 0].reshape(every, LANES)
    krow = lax.broadcasted_iota(jnp.int32, (kept, every), 0)
    kcol = lax.broadcasted_iota(jnp.int32, (kept, every), 1)
    source = (krow // tm) * sr + krow % tm
    pick = jnp.where(kcol == source, 1.0, 0.0).astype(F32)
    mixed_rows = dot(pick, slices, precision=HIGH)
    mapped = dot_split(mixed_rows[:, :rows], wo[...])
    for n in range(dp):
        part[n] = turned(mapped[:, n * rows : (n + 1) * rows])
    go_all(("part",), [
        remote(part.at[(i + r) % dp], part_all.at[i], ("part",), (i + r) % dp, t) for r in range(1, dp)
    ], part_all.at[0 : dp - 1])
    plain_rows = dot(jnp.where(kcol == source + tm, 1.0, 0.0).astype(F32), slices, precision=HIGH)
    part_all[i] = part[i] + turned(plain_rows[:, :rows])
    marks = msg_all[:, 1].reshape(every, LANES)
    table = dot(marks, marks, 0, 0, precision=HIGH)[both : both + n_codes]
    count = jnp.sum(table[:, both : both + n_codes], axis=1, keepdims=True)
    d_pairs = dot(pick, marks, precision=HIGH)
    step_out[...] = table[:, :latent] * (-1.0 / BETA) / count

    landed(("part",), part_all.at[0 : dp - 1])
    final = part_all[0]
    for n in range(1, dp):
        final = final + part_all[n]
    final_all[i] = final
    go_all(("final",), [
        remote(final_all.at[i], final_all.at[i], ("final",), (i + r) % dp, t) for r in range(1, dp)
    ], final_all.at[0 : dp - 1])
    landed(("final",), final_all.at[0 : dp - 1])
    pooled = jnp.concatenate([final_all[n] for n in range(dp)], axis=0 if turn else 1)
    grads = dot(d_pairs, pooled, 0, 1 if turn else 0, precision=HIGH)
    for m in range(2):
        pair_out[m] = grads[m * latent : (m + 1) * latent]

    landed(("done",), out.at[0 : (tm - 1) * mine])
    remote(out.at[0 : (tm - 1) * mine], out.at[0 : (tm - 1) * mine], ("done",), i, t).wait_send()
    settle(started)
    assert len(tags) <= send.shape[0], len(tags)


def write_out(grad, pair, step, grad_out, pair_out, step_out, sem):
    copies = [
        pltpu.make_async_copy(src, dst, sem.at[n])
        for n, (src, dst) in enumerate(((grad, grad_out), (pair, pair_out), (step, step_out)))
    ]
    for copy in copies:
        copy.start()
    for copy in copies:
        copy.wait()


def local(dp, tm, tokens, gain, w_qkv, w_out, w_pair, codebook, codes):
    patches, width = tokens.shape[2:]
    rows = w_qkv.shape[0]
    latent, n_codes = w_pair.shape[2], codebook.shape[0]
    both = 2 * latent
    fp = -(-tm // 8) * 8
    sr = -(-2 * tm // 8) * 8
    lanes = tm * (width // HEAD_DIM)
    pieces = width // 256
    assert rows <= LANES and 2 * both <= LANES and both + n_codes <= LANES
    slab = (rows, dp * tm) if rows % LANES else (dp * tm, rows)
    chips = dp // 2
    tags = (26 if chips == 4 else 2 * dp + 4) + 2 * chips + 8
    vmem = pl.BlockSpec(memory_space=pltpu.VMEM)
    hbm = pl.BlockSpec(memory_space=pltpu.HBM)
    grad, pair, step = pl.pallas_call(
        functools.partial(kernel, (dp, tm, rows, patches, width, latent, n_codes, pieces)),
        out_shape=(
            pltpu.VMEM((patches, width), BF16),
            pltpu.VMEM((2, latent, width), F32),
            pltpu.VMEM((n_codes, latent), F32),
        ),
        in_specs=[hbm] * 7,
        out_specs=(vmem, vmem, vmem),
        scratch_shapes=[
            pltpu.VMEM((dp * rows, 3 * width), BF16),
            pltpu.VMEM((rows, width), BF16),
            pltpu.VMEM((both, width), F32),
            pltpu.VMEM((width,), BF16),
            pltpu.VMEM((n_codes, latent), F32),
            pltpu.SMEM((1, 1, 1), jnp.int32),
            pltpu.VMEM((patches, width), BF16),
            pltpu.VMEM((patches, width), BF16),
            pltpu.VMEM((patches, LANES), F32),
            pltpu.VMEM((patches if 2 * rows % LANES == 0 else 8, 3 * width), F32),
            pltpu.VMEM((patches, 3 * width), BF16),
            pltpu.VMEM((tm * width, lanes), BF16),
            pltpu.VMEM((lanes, width), BF16),
            pltpu.VMEM((patches, lanes), F32),
            pltpu.VMEM((patches, lanes), F32),
            pltpu.VMEM((patches, lanes), BF16),
            pltpu.VMEM((lanes, width), BF16),
            pltpu.VMEM((patches, lanes), F32),
            pltpu.VMEM((patches, LANES), F32),
            pltpu.VMEM((patches, 3 * width), BF16),
            pltpu.VMEM((patches, width), BF16),
            pltpu.VMEM((fp, width), F32),
            pltpu.VMEM((fp, width), F32),
            pltpu.VMEM((3 * both, width), BF16),
            pltpu.VMEM((3 * both, width), BF16),
            pltpu.VMEM((dp, both, rows), F32),
            pltpu.VMEM((fp, LANES), F32),
            pltpu.VMEM((tm, fp, LANES), F32),
            pltpu.VMEM((sr, width), F32),
            pltpu.VMEM((tm, sr, width), F32),
            pltpu.VMEM((dp, 2, sr, LANES), F32),
            pltpu.VMEM((dp, 2, sr, LANES), F32),
            pltpu.VMEM((dp, *slab), F32),
            pltpu.VMEM((dp, *slab), F32),
            pltpu.VMEM((dp, *slab), F32),
            pltpu.SemaphoreType.DMA((tags,)),
            pltpu.SemaphoreType.DMA((tags,)),
            pltpu.SemaphoreType.DMA((10,)),
        ],
        compiler_params=pltpu.CompilerParams(
            collective_id=0, has_side_effects=True, vmem_limit_bytes=60000 * 1024
        ),
    )(
        tokens.reshape(patches, width), gain, w_qkv, w_out, w_pair.swapaxes(1, 2).reshape(both, width), codebook,
        codes,
    )
    made = (grad, pair, step)
    grad, pair, step = pl.pallas_call(
        write_out,
        out_shape=tuple(jax.ShapeDtypeStruct(v.shape, v.dtype) for v in made),
        in_specs=[vmem] * 3,
        out_specs=(hbm, hbm, hbm),
        scratch_shapes=[pltpu.SemaphoreType.DMA((3,))],
        compiler_params=pltpu.CompilerParams(vmem_limit_bytes=4096 * 1024),
    )(*made)
    return grad.reshape(tokens.shape), pair.swapaxes(1, 2), step


def solution(mesh):
    placed = (
        P("dp", "tm", None, None),
        P(),
        P("dp", None),
        P("dp", None),
        P(),
        P(),
        P("dp", "tm", None),
    )
    return jax.shard_map(
        functools.partial(local, mesh.shape["dp"], mesh.shape["tm"]),
        mesh=mesh,
        in_specs=placed,
        out_specs=(P("dp", "tm", None, None), P(), P()),
        check_vma=False,
    )
```

```python
import functools

import jax
import jax.numpy as jnp
from jax import lax
from jax.experimental import pallas as pl
from jax.experimental.pallas import tpu as pltpu
from jax.sharding import PartitionSpec as P

HEAD_DIM = 64
EPS = 1e-06
BETA = 0.25
LANES = 128
F32 = jnp.float32
BF16 = jnp.bfloat16
HIGH = lax.Precision.HIGHEST


def dot(a, b, ca=1, cb=0, precision=None):
    return lax.dot_general(
        a, b, (((ca,), (cb,)), ((), ())), precision=precision, preferred_element_type=F32
    )


def dot_split(a, b, cb=0):
    high = a.astype(BF16)
    rest = a - high.astype(F32)
    mid = rest.astype(BF16)
    low = (rest - mid.astype(F32)).astype(BF16)
    n = a.shape[0]
    terms = jnp.concatenate([high.astype(F32), mid.astype(F32), low.astype(F32)], axis=0)
    out = dot(terms.astype(BF16), b, 1, cb)
    return out[:n] + out[n : 2 * n] + out[2 * n :]


def bits_of(n):
    return max(n.bit_length() - 1, 0)


def ring_place(chip, n):
    b = [(chip // 2**k) % 2 for k in range(bits_of(n))]
    return sum(((sum(b[k:]) % 2) * 2**k for k in range(len(b))), 0)


def ring_chip(place, n):
    count = bits_of(n)
    b = [(place // 2**k) % 2 for k in range(count)] + [0]
    return sum((((b[k] + b[k + 1]) % 2) * 2**k for k in range(count)), 0)


def split2(a):
    high = a.astype(BF16).astype(F32)
    return high, a - high


def reduce_rows(v, parts, n):
    high, mid = split2(v)
    r = dot(jnp.concatenate([high, mid], axis=0).astype(BF16), parts[0 : 2 * n, :], 1, 1)
    r = r[: v.shape[0]] + r[v.shape[0] :]
    return r[:, :n] + r[:, n : 2 * n]


def expand_rows(b, parts):
    high, mid = split2(b)
    return dot(jnp.concatenate([high, high, mid], axis=1).astype(BF16), parts[...])


def three_parts(value):
    high, mid = split2(value)
    return jnp.concatenate([high, mid, high], axis=0).astype(BF16)


def kernel(
    cfg, tokens, gain_in, wq_own, wo_in, wp_in, codebook_in, codes_in,
    out, pair_out, step_out,
    wq, wq_t, wo, wp, gain, codebook, codes, x, normed, scales, acc, qkv, place, lift,
    raw, w_full, w_low, d_big, d_s, slope, dqkv, done, d_rows, d_att,
    wps, mts, mt_all, tile, tile_all, sums, sums_all, msg, msg_all, part, part_all, final_all,
    send, recv, local_sem,
):
    dp, tm, rows, patches, width, latent, n_codes, pieces = cfg
    mine = patches // tm
    total = tm * mine
    sub = 32 if mine % 32 == 0 else mine
    wide = width // pieces
    fp, sr = tile.shape[0], sums.shape[0]
    heads = width // HEAD_DIM
    lanes = tm * heads
    both = 2 * latent
    chips = dp // 2
    half_ring = chips // 2
    i = lax.axis_index("dp")
    t = lax.axis_index("tm")
    core = i % 2
    spot = ring_place(i // 2, chips)

    def device_at(p, c):
        return ring_chip((p + 2 * chips) % chips, chips) * 2 + c

    barrier = pltpu.get_barrier_semaphore()
    for r in range(1, tm):
        pl.semaphore_signal(barrier, inc=1, device_id={"dp": i, "tm": (t + r) % tm})
    for r in range(1, dp):
        pl.semaphore_signal(barrier, inc=1, device_id={"dp": (i + r) % dp, "tm": t})

    def frame_rows(f):
        return pl.ds(pl.multiple_of(f * mine, mine), mine)

    half = rows // 2
    dirs = (1, -1)
    quarter = half // 2
    sharing = half_ring == 2 and quarter % 16 == 0 and tm % 2 == 0
    odd = t % 2
    twin = t + 1 - 2 * odd

    def own_at(at, n):
        return wq_own.at[pl.ds(pl.multiple_of(at, n), n)], wq.at[pl.ds(pl.multiple_of(i * rows + at, n), n)]

    if sharing:
        loads = [
            own_at(h * half + which * quarter, quarter) for which in (odd, 1 - odd) for h in (1, 0)
        ]
    else:
        loads = [own_at(0, rows)]
    loads = [
        pltpu.make_async_copy(src, dst, local_sem.at[6 + n]) for n, (src, dst) in enumerate(loads)
    ]
    here = [
        pltpu.make_async_copy(src, dst, local_sem.at[n])
        for n, (src, dst) in enumerate((
            (wp_in, wp),
            (wo_in, wo),
            (tokens.at[frame_rows(t)], x.at[frame_rows(t)]),
            (gain_in, gain),
            (codebook_in, codebook),
            (codes_in, codes),
        ))
    ]
    for copy in loads + here:
        copy.start()

    col_head = lax.broadcasted_iota(jnp.int32, (width, lanes), 0) // HEAD_DIM
    lane_id = lax.broadcasted_iota(jnp.int32, (width, lanes), 1)
    for f in range(tm):
        place[f * width : (f + 1) * width, :] = jnp.where(lane_id == f * heads + col_head, 1.0, 0.0).astype(BF16)
    row_head = lax.broadcasted_iota(jnp.int32, (lanes, width), 0) % heads
    lift_col = lax.broadcasted_iota(jnp.int32, (lanes, width), 1) // HEAD_DIM
    lift[...] = jnp.where(row_head == lift_col, 1.0, 0.0).astype(BF16)

    tags = {}

    def tag(*key):
        return tags.setdefault(key, len(tags))

    started = []

    def remote(src, dst, key, dpi, tmi):
        k = tag(*key)
        return pltpu.make_async_remote_copy(
            src_ref=src, dst_ref=dst, send_sem=send.at[k], recv_sem=recv.at[k],
            device_id={"dp": dpi, "tm": tmi},
        )

    def go(copy):
        copy.start()
        started.append(copy)

    def go_all(key, copies, landing):
        for copy in copies:
            copy.start()
        started.append(remote(landing, landing, key, i, t))

    def landed(key, landing):
        remote(landing, landing, key, i, t).wait_recv()

    def settle(copies):
        for copy in copies:
            copy.wait_send()

    def piece(origin, h):
        return wq.at[pl.ds(pl.multiple_of(origin * rows + h * half, half), half)]

    def main_half(d):
        return 0 if dirs[d] == 1 else 1

    def halves(d, s):
        first = main_half(d)
        return (first, 1 - first) if s < half_ring - 1 else (first,)

    def quarter_of(origin, h, which):
        at = origin * rows + h * half + which * quarter
        return wq.at[pl.ds(pl.multiple_of(at, quarter), quarter)]

    def ring_copy(d, s, h):
        ref = piece(device_at(spot - dirs[d] * s, core), h)
        return remote(ref, ref, ("ring", d, s, h), device_at(spot + dirs[d], core), t)

    def sib_copy(d, s, h):
        ref = piece(device_at(spot - dirs[d] * s, core), h)
        return remote(ref, ref, ("sib", d, s, h), device_at(spot, 1 - core), t)

    def take(d, s, h):
        ring_copy(d, s, h).wait_recv()
        if s + 1 < half_ring and h in halves(d, s + 1):
            go(ring_copy(d, s + 1, h))
        go(sib_copy(d, s + 1, h))

    def shared_copy(d):
        ref = quarter_of(i, 1 - main_half(d), odd)
        return remote(ref, ref, ("shared", d), device_at(spot + dirs[d], core), t)

    def twin_copy(d):
        at = quarter_of(device_at(spot - dirs[d], core), 1 - main_half(d), odd)
        return remote(at, at, ("twin", d), i, twin)

    def quarter_sib(d, n):
        which = odd if n == 0 else 1 - odd
        at = quarter_of(device_at(spot - dirs[d], core), 1 - main_half(d), which)
        return remote(at, at, ("quarter", d, n), device_at(spot, 1 - core), t)

    def main_copy(d, s, n):
        ref = quarter_of(device_at(spot - dirs[d] * s, core), main_half(d), n)
        return remote(ref, ref, ("main", d, s, n), device_at(spot + dirs[d], core), t)

    def main_sib(d, s, n):
        ref = quarter_of(device_at(spot - dirs[d] * s, core), main_half(d), n)
        return remote(ref, ref, ("mainsib", d, s, n), device_at(spot, 1 - core), t)

    def take_main(d, s, n):
        main_copy(d, s, n).wait_recv()
        if s == 0:
            go(main_copy(d, 1, n))
        go(main_sib(d, s + 1, n))

    map_rows = both // tm if both // tm % 8 == 0 else both

    def map_part(origin):
        if map_rows == both:
            return mt_all.at[origin]
        return mt_all.at[origin, pl.ds(pl.multiple_of(t * map_rows, map_rows), map_rows)]

    def map_copy(k):
        at = mt_all.at[device_at(spot - k, core)]
        return remote(at, at, ("map",), device_at(spot, 1 - core), t)

    def map_far(k):
        at = map_part(i)
        return remote(at, at, ("far", k), device_at(spot + k, core), t)

    def map_near(k, r):
        at = map_part(device_at(spot - k, core))
        return remote(at, at, ("near", k), i, (t + r) % tm)

    near_rows = mt_all.at[0, 0 : (tm - 1) * map_rows] if map_rows != both else None

    def pass_far():
        for k in range(1, chips):
            map_far(k).wait_recv()
            if map_rows != both:
                go_all(("near", k), [map_near(k, r) for r in range(1, tm)], near_rows)

    def pass_near():
        if map_rows != both:
            for k in range(1, chips):
                landed(("near", k), near_rows)
        go_all(("map",), [map_copy(k) for k in range(chips)], mt_all.at[0:chips])

    loads[0].wait()
    pl.semaphore_wait(barrier, tm + dp - 2)
    if sharing:
        go(shared_copy(0))
        loads[1].wait()
        go(shared_copy(1))
        for copy in loads[2:]:
            copy.wait()
        for n in range(2):
            for d in range(2):
                go(main_copy(d, 0, n))
    else:
        for n in range(2):
            for d in range(2):
                if n < len(halves(d, 0)):
                    go(ring_copy(d, 0, halves(d, 0)[n]))
    others = sorted(range(1, tm), key=lambda r: -min(r, tm - r))
    go_all(("tok",), [
        remote(tokens.at[frame_rows((t + r) % tm)], x.at[frame_rows(t)], ("tok",), i, (t + r) % tm) for r in others
    ], x.at[0 : (tm - 1) * mine])
    for h in range(2):
        go(sib_copy(0, 0, h))

    for copy in here:
        copy.wait()
    mt_all[i] = dot_split(wp[...], wo[...], 1)
    for k in range(1, chips):
        go(map_far(k))
    wps[...] = three_parts(wp[...])

    if sharing:
        for d in range(2):
            shared_copy(d).wait_recv()
            go(twin_copy(d))
            go(quarter_sib(d, 0))
        for n in range(2):
            for d in range(2):
                take_main(d, 0, n)
        pass_far()
    elif half_ring > 1:
        for d in range(2):
            take(d, 0, main_half(d))

    landed(("tok",), x.at[0 : (tm - 1) * mine])

    block = 32
    gain_row = gain[...].astype(F32).reshape(1, width)

    def norm_step(b, carry):
        at = pl.ds(pl.multiple_of(b * block, block), block)
        xf = x[at, :].astype(F32)
        scale = lax.rsqrt(jnp.mean(xf * xf, axis=-1, keepdims=True) + EPS)
        scales[at, :] = jnp.broadcast_to(scale, (block, LANES))
        normed[at, :] = (xf * scale * gain_row).astype(BF16)
        return carry

    lax.fori_loop(0, total // block, norm_step, 0)

    frow = lax.broadcasted_iota(jnp.int32, (fp, total), 0)
    fcol = lax.broadcasted_iota(jnp.int32, (fp, total), 1)
    x_sum = dot(jnp.where(fcol // mine == frow, 1.0, 0.0).astype(BF16), x[...])
    sums[...] = jnp.zeros_like(sums)
    sums[tm : 2 * tm, :] = x_sum[:tm]
    trow = lax.broadcasted_iota(jnp.int32, (fp, LANES), 0)
    tlane = lax.broadcasted_iota(jnp.int32, (fp, LANES), 1)
    tile[...] = jnp.where((trow == t) & (tlane == both + codes[0, 0, 0]), 1.0, 0.0).astype(F32)
    x_part = reduce_rows(x_sum, wps, both)

    pair = 2 * rows
    columns = 512

    def project(p, first, last):
        base = pl.multiple_of(ring_chip((p + 2 * chips) % chips, chips) * pair, pair)

        for n in range(3 * width // columns):
            at = slice(n * columns, (n + 1) * columns)
            got = dot(normed[:, pl.ds(base, pair)], wq[pl.ds(base, pair), at])
            if not first:
                got = got + acc[:, at]
            if last:
                qkv[:, at] = got.astype(BF16)
            else:
                acc[:, at] = got

    def wait_sib(d, s, h):
        sib_copy(d, s, h).wait_recv()

    by_chip = pair % LANES == 0

    def flip(p):
        base = pl.multiple_of(ring_chip((p + 2 * chips) % chips, chips) * pair, pair)
        for c in range(0, 3 * width, columns):
            wq_t[c : c + columns, pl.ds(base, pair)] = wq[pl.ds(base, pair), c : c + columns].T

    for h in range(2):
        wait_sib(0, 0, h)
    if by_chip:
        project(spot, True, chips == 1)
        flip(spot)
    if sharing:
        for d in range(2):
            twin_copy(d).wait_recv()
            go(quarter_sib(d, 1))
        pass_near()
        for d in range(2):
            for n in range(2):
                main_sib(d, 1, n).wait_recv()
                quarter_sib(d, n).wait_recv()
            if by_chip:
                project(spot - dirs[d], False, False)
                if d == 1:
                    flip(spot - dirs[0])
            if d == 0:
                for e in range(2):
                    take_main(e, 1, 0)
    else:
        for s in range(half_ring):
            for d in range(2):
                for n, h in enumerate(halves(d, s)):
                    if not (half_ring > 1 and s == 0 and n == 0):
                        take(d, s, h)
            if s < half_ring - 1:
                for d in range(2):
                    for h in halves(d, s):
                        wait_sib(d, s + 1, h)
                    if by_chip:
                        project(spot - dirs[d] * (s + 1), False, False)
                        flip(spot - dirs[d] * (s + 1))

    if not sharing:
        pass_far()
        pass_near()
    landed(("map",), mt_all.at[0:chips])
    mts[...] = three_parts(jnp.concatenate([mt_all[n] for n in range(dp)], axis=1))

    if sharing:
        for d in range(2):
            take_main(d, 1, 1)
        for d in range(2):
            for n in range(2):
                main_sib(d, 2, n).wait_recv()
    else:
        for d in range(2):
            for h in halves(d, half_ring - 1):
                wait_sib(d, half_ring, h)
    if by_chip:
        project(spot + half_ring, False, True)
    else:
        def whole_body(n, carry):
            at = pl.ds(pl.multiple_of(n * columns, columns), columns)
            qkv[:, at] = dot(normed[...], wq[:, at]).astype(BF16)
            return carry

        lax.fori_loop(0, 3 * width // columns, whole_body, 0)

    scale_q = HEAD_DIM ** (-0.5)

    def frame(f):
        return slice(f * mine, (f + 1) * mine)

    scores = [None] * tm
    for f in range(tm):
        q = qkv[frame(f), 0:width]
        products = jnp.concatenate([q] * (f + 1), axis=0) * qkv[0 : (f + 1) * mine, width : 2 * width]
        r = dot(products, place[f * width : (f + 1) * width, :])
        for g in range(f + 1):
            scores[g] = r[frame(g)] if scores[g] is None else scores[g] + r[frame(g)]
    lane_frame = lax.broadcasted_iota(jnp.int32, (mine, lanes), 1) // heads
    for g in range(tm):
        raw[frame(g), :] = scores[g]
    scores = [jnp.where(lane_frame >= g, s * scale_q, -1e30) for g, s in enumerate(scores)]
    top = functools.reduce(jnp.maximum, scores)
    raised = [jnp.exp(s - top) for s in scores]
    whole = functools.reduce(jnp.add, raised)
    for g in range(tm):
        w = raised[g] / whole
        w_full[frame(g), :] = w
        w_low[frame(g), :] = w.astype(BF16)
    mixed = dot(w_low[...], qkv[:, 2 * width :], 0, 0) * lift[...].astype(F32)
    sums[0:tm, :] = jnp.sum(mixed.reshape(tm, heads, width), axis=1)

    tile[:, :both] = (reduce_rows(sums[0:fp, :], mts, both) + x_part) * (1.0 / patches)
    before = list(started)
    started.clear()
    go_all(("tile",), [
        remote(tile, tile_all.at[t], ("tile",), i, (t + r) % tm) for r in others
    ], tile_all.at[0 : tm - 1])
    go_all(("sum",), [
        remote(sums, sums_all.at[t], ("sum",), i, (t + r) % tm) for r in others
    ], sums_all.at[0 : tm - 1])
    tile_all[t] = tile[...]
    sums_all[t] = sums[...]
    if by_chip:
        if sharing:
            flip(spot - dirs[1])
        flip(spot + half_ring)
    else:
        for c in range(0, 3 * width, columns):
            wq_t[c : c + columns, :] = wq[:, c : c + columns].T
    settle(before)
    landed(("tile",), tile_all.at[0 : tm - 1])

    tot = tile_all[0]
    for r in range(1, tm):
        tot = tot + tile_all[r]
    lrow = lax.broadcasted_iota(jnp.int32, (fp, latent), 0)
    following = jnp.where(lrow < tm - 1, pltpu.roll(tot, fp - 1, 0)[:, latent:both], 0.0)
    onehot = tot[:, both : both + n_codes]
    quantized = onehot[:, 0:1] * codebook[0:1, :]
    for n in range(1, n_codes):
        quantized = quantized + onehot[:, n : n + 1] * codebook[n : n + 1, :]
    d_action = jnp.where(lrow < tm, (2.0 * BETA) * (tot[:, :latent] + following - quantized), 0.0)
    earlier = jnp.where((lrow > 0) & (lrow < tm), pltpu.roll(d_action, 1, 0), 0.0)
    d_pair = jnp.concatenate([d_action, earlier], axis=1)
    d_att[...] = expand_rows(d_pair, mts).astype(BF16).astype(F32)
    d_rows[...] = expand_rows(d_pair, wps)

    for f in range(tm):
        at = slice(f * heads, (f + 1) * heads)
        d_big[at, :] = (lift[at, :].astype(F32) * d_att[f : f + 1, :]).astype(BF16)
    d_w = dot(qkv[:, 2 * width :], d_big[...], 1, 1).astype(BF16).astype(F32)
    wd = [w_full[frame(g), :] * d_w[frame(g)] for g in range(tm)]
    mean = functools.reduce(jnp.add, wd)
    through = []
    for g in range(tm):
        d = ((wd[g] - w_full[frame(g), :] * mean) * scale_q).astype(BF16).astype(F32)
        d_s[frame(g), :] = d
        through.append(d * raw[frame(g), :])
    through_all = functools.reduce(jnp.add, through)
    for g in range(tm):
        value = wd[g] + through[g] + jnp.where(lane_frame == g, through_all, 0.0)
        scale = scales[frame(g), 0:1]
        value = jnp.sum(value, axis=-1, keepdims=True) * (1.0 / width) * scale * scale
        slope[frame(g), :] = jnp.broadcast_to(value, (mine, LANES))

    lane_f = lax.broadcasted_iota(jnp.int32, (sub, lanes), 1) // heads
    block_c = 256
    for n in range(mine // sub):
        def own(f):
            return slice(f * mine + n * sub, f * mine + (n + 1) * sub)

        picked = [
            jnp.concatenate([jnp.where(lane_f == f, d_s[own(g), :], 0.0) for g in range(f + 1)], axis=0).astype(BF16)
            for f in range(tm)
        ]
        for c in range(0, width, block_c):
            k = [qkv[own(g), width + c : width + c + block_c].astype(F32) for g in range(tm)]
            dk = [None] * tm
            for f in range(tm):
                q = qkv[own(f), c : c + block_c].astype(F32)
                spread = dot(picked[f], lift[:, c : c + block_c])
                dq = None
                for g in range(f + 1):
                    v = spread[g * sub : (g + 1) * sub]
                    dq = v * k[g] if dq is None else dq + v * k[g]
                    dk[g] = v * q if dk[g] is None else dk[g] + v * q
                dqkv[own(f), c : c + block_c] = dq.astype(BF16)
            for g in range(tm):
                dqkv[own(g), width + c : width + c + block_c] = dk[g].astype(BF16)
    dqkv[:, 2 * width :] = dot(w_low[...], d_big[...]).astype(BF16)

    def done_copy(n, r, other):
        at = pl.ds(n * wide, wide)
        return remote(done.at[frame_rows(other), at], out.at[frame_rows(t), at], ("done",), i, other)

    def give(n):
        at = slice(n * wide, (n + 1) * wide)
        mid = total // 2
        dn = jnp.concatenate([dot(dqkv[:mid, :], wq_t[:, at]), dot(dqkv[mid:, :], wq_t[:, at])], axis=0)
        dn = dn.astype(BF16).astype(F32)
        for f in range(tm):
            u = dn[frame(f)] * gain_row[:, at]
            dx = u * scales[frame(f), 0:1] - x[frame(f), at].astype(F32) * slope[frame(f), 0:1]
            done[frame(f), at] = (d_rows[f : f + 1, at] + dx).astype(BF16)
        for r in others:
            done_copy(n, r, (t + r) % tm).start()
        out[frame_rows(t), at] = done[frame_rows(t), at]

    def share():
        landed(("sum",), sums_all.at[0 : tm - 1])
        s = sums_all[0]
        for r in range(1, tm):
            s = s + sums_all[r]
        s = s * (1.0 / patches)
        for n in range(dp):
            msg[n] = jnp.zeros_like(msg[n])
            msg[n, 0, :, 0:rows] = s[:, n * rows : (n + 1) * rows]
            msg[n, 1, 0:tm, 0:both] = d_pair[:tm]
            msg[n, 1, 0:tm, both : both + n_codes] = onehot[:tm]
        go_all(("msg",), [
            remote(msg.at[(i + r) % dp], msg_all.at[i], ("msg",), (i + r) % dp, t) for r in range(1, dp)
        ], msg_all.at[0 : dp - 1])
        msg_all[i] = msg[i]

    give(0)
    share()
    for n in range(1, pieces):
        give(n)

    landed(("msg",), msg_all.at[0 : dp - 1])
    turn = rows % LANES != 0

    def turned(v):
        return v.T if turn else v

    every = dp * sr
    kept = dp * tm
    slices = msg_all[:, 0].reshape(every, LANES)
    krow = lax.broadcasted_iota(jnp.int32, (kept, every), 0)
    kcol = lax.broadcasted_iota(jnp.int32, (kept, every), 1)
    source = (krow // tm) * sr + krow % tm
    pick = jnp.where(kcol == source, 1.0, 0.0).astype(F32)
    mixed_rows = dot(pick, slices, precision=HIGH)
    mapped = dot_split(mixed_rows[:, :rows], wo[...])
    for n in range(dp):
        part[n] = turned(mapped[:, n * rows : (n + 1) * rows])
    go_all(("part",), [
        remote(part.at[(i + r) % dp], part_all.at[i], ("part",), (i + r) % dp, t) for r in range(1, dp)
    ], part_all.at[0 : dp - 1])
    plain_rows = dot(jnp.where(kcol == source + tm, 1.0, 0.0).astype(F32), slices, precision=HIGH)
    part_all[i] = part[i] + turned(plain_rows[:, :rows])
    marks = msg_all[:, 1].reshape(every, LANES)
    table = dot(marks, marks, 0, 0, precision=HIGH)[both : both + n_codes]
    count = jnp.sum(table[:, both : both + n_codes], axis=1, keepdims=True)
    d_pairs = dot(pick, marks, precision=HIGH)
    step_out[...] = table[:, :latent] * (-1.0 / BETA) / count

    landed(("part",), part_all.at[0 : dp - 1])
    final = part_all[0]
    for n in range(1, dp):
        final = final + part_all[n]
    final_all[i] = final
    go_all(("final",), [
        remote(final_all.at[i], final_all.at[i], ("final",), (i + r) % dp, t) for r in range(1, dp)
    ], final_all.at[0 : dp - 1])
    landed(("final",), final_all.at[0 : dp - 1])
    pooled = jnp.concatenate([final_all[n] for n in range(dp)], axis=0 if turn else 1)
    grads = dot(d_pairs, pooled, 0, 1 if turn else 0, precision=HIGH)
    for m in range(2):
        pair_out[m] = grads[m * latent : (m + 1) * latent]

    landed(("done",), out.at[0 : (tm - 1) * mine])
    remote(out.at[0 : (tm - 1) * mine], out.at[0 : (tm - 1) * mine], ("done",), i, t).wait_send()
    settle(started)
    assert len(tags) <= send.shape[0], len(tags)


def write_out(grad, pair, step, grad_out, pair_out, step_out, sem):
    chunk = grad.shape[0] // 4
    parts = [pl.ds(n * chunk, chunk) for n in range(4)]
    copies = [
        pltpu.make_async_copy(src, dst, sem.at[n])
        for n, (src, dst) in enumerate(
            [(grad.at[part], grad_out.at[part]) for part in parts] + [(pair, pair_out), (step, step_out)]
        )
    ]
    for copy in copies:
        copy.start()
    for copy in copies:
        copy.wait()


def local(dp, tm, tokens, gain, w_qkv, w_out, w_pair, codebook, codes):
    patches, width = tokens.shape[2:]
    rows = w_qkv.shape[0]
    latent, n_codes = w_pair.shape[2], codebook.shape[0]
    both = 2 * latent
    fp = -(-tm // 8) * 8
    sr = -(-2 * tm // 8) * 8
    lanes = tm * (width // HEAD_DIM)
    pieces = width // 256
    assert rows <= LANES and 2 * both <= LANES and both + n_codes <= LANES
    slab = (rows, dp * tm) if rows % LANES else (dp * tm, rows)
    chips = dp // 2
    tags = (26 if chips == 4 else 2 * dp + 4) + 2 * chips + 8
    vmem = pl.BlockSpec(memory_space=pltpu.VMEM)
    hbm = pl.BlockSpec(memory_space=pltpu.HBM)
    grad, pair, step = pl.pallas_call(
        functools.partial(kernel, (dp, tm, rows, patches, width, latent, n_codes, pieces)),
        out_shape=(
            pltpu.VMEM((patches, width), BF16),
            pltpu.VMEM((2, latent, width), F32),
            pltpu.VMEM((n_codes, latent), F32),
        ),
        in_specs=[hbm] * 7,
        out_specs=(vmem, vmem, vmem),
        scratch_shapes=[
            pltpu.VMEM((dp * rows, 3 * width), BF16),
            pltpu.VMEM((3 * width, dp * rows), BF16),
            pltpu.VMEM((rows, width), BF16),
            pltpu.VMEM((both, width), F32),
            pltpu.VMEM((width,), BF16),
            pltpu.VMEM((n_codes, latent), F32),
            pltpu.SMEM((1, 1, 1), jnp.int32),
            pltpu.VMEM((patches, width), BF16),
            pltpu.VMEM((patches, width), BF16),
            pltpu.VMEM((patches, LANES), F32),
            pltpu.VMEM((patches if 2 * rows % LANES == 0 else 8, 3 * width), F32),
            pltpu.VMEM((patches, 3 * width), BF16),
            pltpu.VMEM((tm * width, lanes), BF16),
            pltpu.VMEM((lanes, width), BF16),
            pltpu.VMEM((patches, lanes), F32),
            pltpu.VMEM((patches, lanes), F32),
            pltpu.VMEM((patches, lanes), BF16),
            pltpu.VMEM((lanes, width), BF16),
            pltpu.VMEM((patches, lanes), F32),
            pltpu.VMEM((patches, LANES), F32),
            pltpu.VMEM((patches, 3 * width), BF16),
            pltpu.VMEM((patches, width), BF16),
            pltpu.VMEM((fp, width), F32),
            pltpu.VMEM((fp, width), F32),
            pltpu.VMEM((3 * both, width), BF16),
            pltpu.VMEM((3 * both, width), BF16),
            pltpu.VMEM((dp, both, rows), F32),
            pltpu.VMEM((fp, LANES), F32),
            pltpu.VMEM((tm, fp, LANES), F32),
            pltpu.VMEM((sr, width), F32),
            pltpu.VMEM((tm, sr, width), F32),
            pltpu.VMEM((dp, 2, sr, LANES), F32),
            pltpu.VMEM((dp, 2, sr, LANES), F32),
            pltpu.VMEM((dp, *slab), F32),
            pltpu.VMEM((dp, *slab), F32),
            pltpu.VMEM((dp, *slab), F32),
            pltpu.SemaphoreType.DMA((tags,)),
            pltpu.SemaphoreType.DMA((tags,)),
            pltpu.SemaphoreType.DMA((10,)),
        ],
        compiler_params=pltpu.CompilerParams(
            collective_id=0, has_side_effects=True, vmem_limit_bytes=60000 * 1024
        ),
    )(
        tokens.reshape(patches, width), gain, w_qkv, w_out, w_pair.swapaxes(1, 2).reshape(both, width), codebook,
        codes,
    )
    made = (grad, pair, step)
    grad, pair, step = pl.pallas_call(
        write_out,
        out_shape=tuple(jax.ShapeDtypeStruct(v.shape, v.dtype) for v in made),
        in_specs=[vmem] * 3,
        out_specs=(hbm, hbm, hbm),
        scratch_shapes=[pltpu.SemaphoreType.DMA((6,))],
        compiler_params=pltpu.CompilerParams(vmem_limit_bytes=4096 * 1024),
    )(*made)
    return grad.reshape(tokens.shape), pair.swapaxes(1, 2), step


def solution(mesh):
    placed = (
        P("dp", "tm", None, None),
        P(),
        P("dp", None),
        P("dp", None),
        P(),
        P(),
        P("dp", "tm", None),
    )
    return jax.shard_map(
        functools.partial(local, mesh.shape["dp"], mesh.shape["tm"]),
        mesh=mesh,
        in_specs=placed,
        out_specs=(P("dp", "tm", None, None), P(), P()),
        check_vma=False,
    )
```

```python
import functools

import jax
import jax.numpy as jnp
from jax import lax
from jax.experimental import pallas as pl
from jax.experimental.pallas import tpu as pltpu
from jax.sharding import PartitionSpec as P

HEAD_DIM = 64
EPS = 1e-06
BETA = 0.25
LANES = 128
F32 = jnp.float32
BF16 = jnp.bfloat16
HIGH = lax.Precision.HIGHEST


def dot(a, b, ca=1, cb=0, precision=None):
    return lax.dot_general(
        a, b, (((ca,), (cb,)), ((), ())), precision=precision, preferred_element_type=F32
    )


def dot_split(a, b, cb=0):
    high = a.astype(BF16)
    rest = a - high.astype(F32)
    mid = rest.astype(BF16)
    low = (rest - mid.astype(F32)).astype(BF16)
    n = a.shape[0]
    terms = jnp.concatenate([high.astype(F32), mid.astype(F32), low.astype(F32)], axis=0)
    out = dot(terms.astype(BF16), b, 1, cb)
    return out[:n] + out[n : 2 * n] + out[2 * n :]


def bits_of(n):
    return max(n.bit_length() - 1, 0)


def ring_place(chip, n):
    b = [(chip // 2**k) % 2 for k in range(bits_of(n))]
    return sum(((sum(b[k:]) % 2) * 2**k for k in range(len(b))), 0)


def ring_chip(place, n):
    count = bits_of(n)
    b = [(place // 2**k) % 2 for k in range(count)] + [0]
    return sum((((b[k] + b[k + 1]) % 2) * 2**k for k in range(count)), 0)


def split2(a):
    high = a.astype(BF16).astype(F32)
    return high, a - high


def reduce_rows(v, parts, n):
    high, mid = split2(v)
    r = dot(jnp.concatenate([high, mid], axis=0).astype(BF16), parts[0 : 2 * n, :], 1, 1)
    r = r[: v.shape[0]] + r[v.shape[0] :]
    return r[:, :n] + r[:, n : 2 * n]


def expand_rows(b, parts):
    high, mid = split2(b)
    return dot(jnp.concatenate([high, high, mid], axis=1).astype(BF16), parts[...])


def three_parts(value):
    high, mid = split2(value)
    return jnp.concatenate([high, mid, high], axis=0).astype(BF16)


def kernel(
    cfg, tokens, gain_in, wq_own, wo_in, wp_in, codebook_in, codes_in,
    out, pair_out, step_out,
    wq, wq_t, wo, wp, gain, codebook, codes, x, normed, scales, acc, qkv, place, lift,
    raw, w_full, w_low, d_big, d_s, slope, dqkv, done, d_rows, d_att,
    wps, mts, mt_all, tile, tile_all, sums, sums_all, msg, msg_all, part, part_all, final_all,
    send, recv, local_sem,
):
    dp, tm, rows, patches, width, latent, n_codes, pieces = cfg
    mine = patches // tm
    total = tm * mine
    sub = 32 if mine % 32 == 0 else mine
    wide = width // pieces
    fp, sr = tile.shape[0], sums.shape[0]
    heads = width // HEAD_DIM
    lanes = tm * heads
    both = 2 * latent
    chips = dp // 2
    half_ring = chips // 2
    i = lax.axis_index("dp")
    t = lax.axis_index("tm")
    core = i % 2
    spot = ring_place(i // 2, chips)

    def device_at(p, c):
        return ring_chip((p + 2 * chips) % chips, chips) * 2 + c

    barrier = pltpu.get_barrier_semaphore()
    for r in range(1, tm):
        pl.semaphore_signal(barrier, inc=1, device_id={"dp": i, "tm": (t + r) % tm})
    for r in range(1, dp):
        pl.semaphore_signal(barrier, inc=1, device_id={"dp": (i + r) % dp, "tm": t})

    def frame_rows(f):
        return pl.ds(pl.multiple_of(f * mine, mine), mine)

    half = rows // 2
    dirs = (1, -1)
    quarter = half // 2
    sharing = half_ring == 2 and quarter % 16 == 0 and tm % 2 == 0
    odd = t % 2
    twin = t + 1 - 2 * odd

    def own_at(at, n):
        return wq_own.at[pl.ds(pl.multiple_of(at, n), n)], wq.at[pl.ds(pl.multiple_of(i * rows + at, n), n)]

    if sharing:
        loads = [
            own_at(h * half + which * quarter, quarter) for which in (odd, 1 - odd) for h in (1, 0)
        ]
    else:
        loads = [own_at(0, rows)]
    loads = [
        pltpu.make_async_copy(src, dst, local_sem.at[6 + n]) for n, (src, dst) in enumerate(loads)
    ]
    here = [
        pltpu.make_async_copy(src, dst, local_sem.at[n])
        for n, (src, dst) in enumerate((
            (wp_in, wp),
            (wo_in, wo),
            (tokens.at[frame_rows(t)], x.at[frame_rows(t)]),
            (gain_in, gain),
            (codebook_in, codebook),
            (codes_in, codes),
        ))
    ]
    for copy in loads + here:
        copy.start()

    col_head = lax.broadcasted_iota(jnp.int32, (width, lanes), 0) // HEAD_DIM
    lane_id = lax.broadcasted_iota(jnp.int32, (width, lanes), 1)
    for f in range(tm):
        place[f * width : (f + 1) * width, :] = jnp.where(lane_id == f * heads + col_head, 1.0, 0.0).astype(BF16)
    row_head = lax.broadcasted_iota(jnp.int32, (lanes, width), 0) % heads
    lift_col = lax.broadcasted_iota(jnp.int32, (lanes, width), 1) // HEAD_DIM
    lift[...] = jnp.where(row_head == lift_col, 1.0, 0.0).astype(BF16)

    tags = {}

    def tag(*key):
        return tags.setdefault(key, len(tags))

    started = []

    def remote(src, dst, key, dpi, tmi):
        k = tag(*key)
        return pltpu.make_async_remote_copy(
            src_ref=src, dst_ref=dst, send_sem=send.at[k], recv_sem=recv.at[k],
            device_id={"dp": dpi, "tm": tmi},
        )

    def go(copy):
        copy.start()
        started.append(copy)

    def go_all(key, copies, landing):
        for copy in copies:
            copy.start()
        started.append(remote(landing, landing, key, i, t))

    def landed(key, landing):
        remote(landing, landing, key, i, t).wait_recv()

    def settle(copies):
        for copy in copies:
            copy.wait_send()

    def piece(origin, h):
        return wq.at[pl.ds(pl.multiple_of(origin * rows + h * half, half), half)]

    def main_half(d):
        return 0 if dirs[d] == 1 else 1

    def halves(d, s):
        first = main_half(d)
        return (first, 1 - first) if s < half_ring - 1 else (first,)

    def quarter_of(origin, h, which):
        at = origin * rows + h * half + which * quarter
        return wq.at[pl.ds(pl.multiple_of(at, quarter), quarter)]

    def ring_copy(d, s, h):
        ref = piece(device_at(spot - dirs[d] * s, core), h)
        return remote(ref, ref, ("ring", d, s, h), device_at(spot + dirs[d], core), t)

    def sib_copy(d, s, h):
        ref = piece(device_at(spot - dirs[d] * s, core), h)
        return remote(ref, ref, ("sib", d, s, h), device_at(spot, 1 - core), t)

    def take(d, s, h):
        ring_copy(d, s, h).wait_recv()
        if s + 1 < half_ring and h in halves(d, s + 1):
            go(ring_copy(d, s + 1, h))
        go(sib_copy(d, s + 1, h))

    def shared_copy(d):
        ref = quarter_of(i, 1 - main_half(d), odd)
        return remote(ref, ref, ("shared", d), device_at(spot + dirs[d], core), t)

    def twin_copy(d):
        at = quarter_of(device_at(spot - dirs[d], core), 1 - main_half(d), odd)
        return remote(at, at, ("twin", d), i, twin)

    def quarter_sib(d, n):
        which = odd if n == 0 else 1 - odd
        at = quarter_of(device_at(spot - dirs[d], core), 1 - main_half(d), which)
        return remote(at, at, ("quarter", d, n), device_at(spot, 1 - core), t)

    def main_copy(d, s, n):
        ref = quarter_of(device_at(spot - dirs[d] * s, core), main_half(d), n)
        return remote(ref, ref, ("main", d, s, n), device_at(spot + dirs[d], core), t)

    def main_sib(d, s, n):
        ref = quarter_of(device_at(spot - dirs[d] * s, core), main_half(d), n)
        return remote(ref, ref, ("mainsib", d, s, n), device_at(spot, 1 - core), t)

    def take_main(d, s, n):
        main_copy(d, s, n).wait_recv()
        if s == 0:
            go(main_copy(d, 1, n))
        go(main_sib(d, s + 1, n))

    map_rows = both // tm if both // tm % 8 == 0 else both

    def map_part(origin):
        if map_rows == both:
            return mt_all.at[origin]
        return mt_all.at[origin, pl.ds(pl.multiple_of(t * map_rows, map_rows), map_rows)]

    def map_copy(k):
        at = mt_all.at[device_at(spot - k, core)]
        return remote(at, at, ("map",), device_at(spot, 1 - core), t)

    def map_far(k):
        at = map_part(i)
        return remote(at, at, ("far", k), device_at(spot + k, core), t)

    def map_near(k, r):
        at = map_part(device_at(spot - k, core))
        return remote(at, at, ("near", k), i, (t + r) % tm)

    near_rows = mt_all.at[0, 0 : (tm - 1) * map_rows] if map_rows != both else None

    def pass_far():
        for k in range(1, chips):
            map_far(k).wait_recv()
            if map_rows != both:
                go_all(("near", k), [map_near(k, r) for r in range(1, tm)], near_rows)

    def pass_near():
        if map_rows != both:
            for k in range(1, chips):
                landed(("near", k), near_rows)
        go_all(("map",), [map_copy(k) for k in range(chips)], mt_all.at[0:chips])

    loads[0].wait()
    pl.semaphore_wait(barrier, tm + dp - 2)
    if sharing:
        go(shared_copy(0))
        loads[1].wait()
        go(shared_copy(1))
        for copy in loads[2:]:
            copy.wait()
        for n in range(2):
            for d in range(2):
                go(main_copy(d, 0, n))
    else:
        for n in range(2):
            for d in range(2):
                if n < len(halves(d, 0)):
                    go(ring_copy(d, 0, halves(d, 0)[n]))
    upper = (2 * t) // tm
    others = [r + upper * (tm - 2 * r) for r in sorted(range(1, tm), key=lambda r: -min(r, tm - r))]
    go_all(("tok",), [
        remote(tokens.at[frame_rows((t + r) % tm)], x.at[frame_rows(t)], ("tok",), i, (t + r) % tm) for r in others
    ], x.at[0 : (tm - 1) * mine])
    for h in range(2):
        go(sib_copy(0, 0, h))

    for copy in here:
        copy.wait()
    mt_all[i] = dot_split(wp[...], wo[...], 1)
    for k in range(1, chips):
        go(map_far(k))
    wps[...] = three_parts(wp[...])

    if sharing:
        for d in range(2):
            shared_copy(d).wait_recv()
            go(twin_copy(d))
            go(quarter_sib(d, 0))
        for n in range(2):
            for d in range(2):
                take_main(d, 0, n)
        pass_far()
    elif half_ring > 1:
        for d in range(2):
            take(d, 0, main_half(d))

    landed(("tok",), x.at[0 : (tm - 1) * mine])

    block = 32
    gain_row = gain[...].astype(F32).reshape(1, width)

    def norm_step(b, carry):
        at = pl.ds(pl.multiple_of(b * block, block), block)
        xf = x[at, :].astype(F32)
        scale = lax.rsqrt(jnp.mean(xf * xf, axis=-1, keepdims=True) + EPS)
        scales[at, :] = jnp.broadcast_to(scale, (block, LANES))
        normed[at, :] = (xf * scale * gain_row).astype(BF16)
        return carry

    lax.fori_loop(0, total // block, norm_step, 0)

    frow = lax.broadcasted_iota(jnp.int32, (fp, total), 0)
    fcol = lax.broadcasted_iota(jnp.int32, (fp, total), 1)
    x_sum = dot(jnp.where(fcol // mine == frow, 1.0, 0.0).astype(BF16), x[...])
    sums[...] = jnp.zeros_like(sums)
    sums[tm : 2 * tm, :] = x_sum[:tm]
    trow = lax.broadcasted_iota(jnp.int32, (fp, LANES), 0)
    tlane = lax.broadcasted_iota(jnp.int32, (fp, LANES), 1)
    tile[...] = jnp.where((trow == t) & (tlane == both + codes[0, 0, 0]), 1.0, 0.0).astype(F32)
    x_part = reduce_rows(x_sum, wps, both)

    pair = 2 * rows
    columns = 512

    def project(p, first, last):
        base = pl.multiple_of(ring_chip((p + 2 * chips) % chips, chips) * pair, pair)

        for n in range(3 * width // columns):
            at = slice(n * columns, (n + 1) * columns)
            got = dot(normed[:, pl.ds(base, pair)], wq[pl.ds(base, pair), at])
            if not first:
                got = got + acc[:, at]
            if last:
                qkv[:, at] = got.astype(BF16)
            else:
                acc[:, at] = got

    def wait_sib(d, s, h):
        sib_copy(d, s, h).wait_recv()

    by_chip = pair % LANES == 0

    def flip(p):
        base = pl.multiple_of(ring_chip((p + 2 * chips) % chips, chips) * pair, pair)
        for c in range(0, 3 * width, columns):
            wq_t[c : c + columns, pl.ds(base, pair)] = wq[pl.ds(base, pair), c : c + columns].T

    for h in range(2):
        wait_sib(0, 0, h)
    if by_chip:
        project(spot, True, chips == 1)
        flip(spot)
    if sharing:
        for d in range(2):
            twin_copy(d).wait_recv()
            go(quarter_sib(d, 1))
        pass_near()
        for d in range(2):
            for n in range(2):
                main_sib(d, 1, n).wait_recv()
                quarter_sib(d, n).wait_recv()
            if by_chip:
                project(spot - dirs[d], False, False)
                if d == 1:
                    flip(spot - dirs[0])
            if d == 0:
                for e in range(2):
                    take_main(e, 1, 0)
    else:
        for s in range(half_ring):
            for d in range(2):
                for n, h in enumerate(halves(d, s)):
                    if not (half_ring > 1 and s == 0 and n == 0):
                        take(d, s, h)
            if s < half_ring - 1:
                for d in range(2):
                    for h in halves(d, s):
                        wait_sib(d, s + 1, h)
                    if by_chip:
                        project(spot - dirs[d] * (s + 1), False, False)
                        flip(spot - dirs[d] * (s + 1))

    if not sharing:
        pass_far()
        pass_near()
    landed(("map",), mt_all.at[0:chips])
    mts[...] = three_parts(jnp.concatenate([mt_all[n] for n in range(dp)], axis=1))

    if sharing:
        for d in range(2):
            take_main(d, 1, 1)
        for d in range(2):
            for n in range(2):
                main_sib(d, 2, n).wait_recv()
    else:
        for d in range(2):
            for h in halves(d, half_ring - 1):
                wait_sib(d, half_ring, h)
    if by_chip:
        project(spot + half_ring, False, True)
    else:
        def whole_body(n, carry):
            at = pl.ds(pl.multiple_of(n * columns, columns), columns)
            qkv[:, at] = dot(normed[...], wq[:, at]).astype(BF16)
            return carry

        lax.fori_loop(0, 3 * width // columns, whole_body, 0)

    scale_q = HEAD_DIM ** (-0.5)

    def frame(f):
        return slice(f * mine, (f + 1) * mine)

    scores = [None] * tm
    for f in range(tm):
        q = qkv[frame(f), 0:width]
        products = jnp.concatenate([q] * (f + 1), axis=0) * qkv[0 : (f + 1) * mine, width : 2 * width]
        r = dot(products, place[f * width : (f + 1) * width, :])
        for g in range(f + 1):
            scores[g] = r[frame(g)] if scores[g] is None else scores[g] + r[frame(g)]
    lane_frame = lax.broadcasted_iota(jnp.int32, (mine, lanes), 1) // heads
    for g in range(tm):
        raw[frame(g), :] = scores[g]
    scores = [jnp.where(lane_frame >= g, s * scale_q, -1e30) for g, s in enumerate(scores)]
    top = functools.reduce(jnp.maximum, scores)
    raised = [jnp.exp(s - top) for s in scores]
    whole = functools.reduce(jnp.add, raised)
    for g in range(tm):
        w = raised[g] / whole
        w_full[frame(g), :] = w
        w_low[frame(g), :] = w.astype(BF16)
    mixed = dot(w_low[...], qkv[:, 2 * width :], 0, 0) * lift[...].astype(F32)
    sums[0:tm, :] = jnp.sum(mixed.reshape(tm, heads, width), axis=1)

    tile[:, :both] = (reduce_rows(sums[0:fp, :], mts, both) + x_part) * (1.0 / patches)
    before = list(started)
    started.clear()
    go_all(("tile",), [
        remote(tile, tile_all.at[t], ("tile",), i, (t + r) % tm) for r in others
    ], tile_all.at[0 : tm - 1])
    go_all(("sum",), [
        remote(sums, sums_all.at[t], ("sum",), i, (t + r) % tm) for r in others
    ], sums_all.at[0 : tm - 1])
    tile_all[t] = tile[...]
    sums_all[t] = sums[...]
    if by_chip:
        if sharing:
            flip(spot - dirs[1])
        flip(spot + half_ring)
    else:
        for c in range(0, 3 * width, columns):
            wq_t[c : c + columns, :] = wq[:, c : c + columns].T
    settle(before)
    landed(("tile",), tile_all.at[0 : tm - 1])

    tot = tile_all[0]
    for r in range(1, tm):
        tot = tot + tile_all[r]
    lrow = lax.broadcasted_iota(jnp.int32, (fp, latent), 0)
    following = jnp.where(lrow < tm - 1, pltpu.roll(tot, fp - 1, 0)[:, latent:both], 0.0)
    onehot = tot[:, both : both + n_codes]
    quantized = onehot[:, 0:1] * codebook[0:1, :]
    for n in range(1, n_codes):
        quantized = quantized + onehot[:, n : n + 1] * codebook[n : n + 1, :]
    d_action = jnp.where(lrow < tm, (2.0 * BETA) * (tot[:, :latent] + following - quantized), 0.0)
    earlier = jnp.where((lrow > 0) & (lrow < tm), pltpu.roll(d_action, 1, 0), 0.0)
    d_pair = jnp.concatenate([d_action, earlier], axis=1)
    d_att[...] = expand_rows(d_pair, mts).astype(BF16).astype(F32)
    d_rows[...] = expand_rows(d_pair, wps)

    for f in range(tm):
        at = slice(f * heads, (f + 1) * heads)
        d_big[at, :] = (lift[at, :].astype(F32) * d_att[f : f + 1, :]).astype(BF16)
    d_w = jnp.concatenate(
        [dot(qkv[at, 2 * width :], d_big[...], 1, 1) for at in (slice(0, total // 2), slice(total // 2, total))], axis=0
    ).astype(BF16).astype(F32)
    wd = [w_full[frame(g), :] * d_w[frame(g)] for g in range(tm)]
    mean = functools.reduce(jnp.add, wd)
    through = []
    for g in range(tm):
        d = ((wd[g] - w_full[frame(g), :] * mean) * scale_q).astype(BF16).astype(F32)
        d_s[frame(g), :] = d
        through.append(d * raw[frame(g), :])
    through_all = functools.reduce(jnp.add, through)
    for g in range(tm):
        value = wd[g] + through[g] + jnp.where(lane_frame == g, through_all, 0.0)
        scale = scales[frame(g), 0:1]
        value = jnp.sum(value, axis=-1, keepdims=True) * (1.0 / width) * scale * scale
        slope[frame(g), :] = jnp.broadcast_to(value, (mine, LANES))

    lane_f = lax.broadcasted_iota(jnp.int32, (sub, lanes), 1) // heads
    block_c = 256
    for n in range(mine // sub):
        def own(f):
            return slice(f * mine + n * sub, f * mine + (n + 1) * sub)

        picked = [
            jnp.concatenate([jnp.where(lane_f == f, d_s[own(g), :], 0.0) for g in range(f + 1)], axis=0).astype(BF16)
            for f in range(tm)
        ]
        for c in range(0, width, block_c):
            k = [qkv[own(g), width + c : width + c + block_c].astype(F32) for g in range(tm)]
            dk = [None] * tm
            for f in range(tm):
                q = qkv[own(f), c : c + block_c].astype(F32)
                spread = dot(picked[f], lift[:, c : c + block_c])
                dq = None
                for g in range(f + 1):
                    v = spread[g * sub : (g + 1) * sub]
                    dq = v * k[g] if dq is None else dq + v * k[g]
                    dk[g] = v * q if dk[g] is None else dk[g] + v * q
                dqkv[own(f), c : c + block_c] = dq.astype(BF16)
            for g in range(tm):
                dqkv[own(g), width + c : width + c + block_c] = dk[g].astype(BF16)
    dqkv[:, 2 * width :] = dot(w_low[...], d_big[...]).astype(BF16)

    def done_copy(n, other):
        at = pl.ds(n * wide, wide)
        return remote(done.at[frame_rows(other), at], out.at[frame_rows(t), at], ("done",), i, other)

    def give(n):
        at = slice(n * wide, (n + 1) * wide)
        mid = total // 2
        dn = jnp.concatenate([dot(dqkv[:mid, :], wq_t[:, at]), dot(dqkv[mid:, :], wq_t[:, at])], axis=0)
        dn = dn.astype(BF16).astype(F32)
        for f in range(tm):
            u = dn[frame(f)] * gain_row[:, at]
            dx = u * scales[frame(f), 0:1] - x[frame(f), at].astype(F32) * slope[frame(f), 0:1]
            done[frame(f), at] = (d_rows[f : f + 1, at] + dx).astype(BF16)
        for r in others:
            done_copy(n, (t + r) % tm).start()
        out[frame_rows(t), at] = done[frame_rows(t), at]

    def share():
        landed(("sum",), sums_all.at[0 : tm - 1])
        s = sums_all[0]
        for r in range(1, tm):
            s = s + sums_all[r]
        s = s * (1.0 / patches)
        for n in range(dp):
            msg[n] = jnp.zeros_like(msg[n])
            msg[n, 0, :, 0:rows] = s[:, n * rows : (n + 1) * rows]
            msg[n, 1, 0:tm, 0:both] = d_pair[:tm]
            msg[n, 1, 0:tm, both : both + n_codes] = onehot[:tm]
        go_all(("msg",), [
            remote(msg.at[(i + r) % dp], msg_all.at[i], ("msg",), (i + r) % dp, t) for r in range(1, dp)
        ], msg_all.at[0 : dp - 1])
        msg_all[i] = msg[i]

    give(0)
    share()
    for n in range(1, pieces):
        give(n)

    landed(("msg",), msg_all.at[0 : dp - 1])
    turn = rows % LANES != 0

    def turned(v):
        return v.T if turn else v

    every = dp * sr
    kept = dp * tm
    slices = msg_all[:, 0].reshape(every, LANES)
    krow = lax.broadcasted_iota(jnp.int32, (kept, every), 0)
    kcol = lax.broadcasted_iota(jnp.int32, (kept, every), 1)
    source = (krow // tm) * sr + krow % tm
    pick = jnp.where(kcol == source, 1.0, 0.0).astype(F32)
    mixed_rows = dot(pick, slices, precision=HIGH)
    mapped = dot_split(mixed_rows[:, :rows], wo[...])
    for n in range(dp):
        part[n] = turned(mapped[:, n * rows : (n + 1) * rows])
    go_all(("part",), [
        remote(part.at[(i + r) % dp], part_all.at[i], ("part",), (i + r) % dp, t) for r in range(1, dp)
    ], part_all.at[0 : dp - 1])
    plain_rows = dot(jnp.where(kcol == source + tm, 1.0, 0.0).astype(F32), slices, precision=HIGH)
    part_all[i] = part[i] + turned(plain_rows[:, :rows])
    marks = msg_all[:, 1].reshape(every, LANES)
    table = dot(marks, marks, 0, 0, precision=HIGH)[both : both + n_codes]
    count = jnp.sum(table[:, both : both + n_codes], axis=1, keepdims=True)
    d_pairs = dot(pick, marks, precision=HIGH)
    step_out[...] = table[:, :latent] * (-1.0 / BETA) / count

    landed(("part",), part_all.at[0 : dp - 1])
    final = part_all[0]
    for n in range(1, dp):
        final = final + part_all[n]
    final_all[i] = final
    go_all(("final",), [
        remote(final_all.at[i], final_all.at[i], ("final",), (i + r) % dp, t) for r in range(1, dp)
    ], final_all.at[0 : dp - 1])
    landed(("final",), final_all.at[0 : dp - 1])
    pooled = jnp.concatenate([final_all[n] for n in range(dp)], axis=0 if turn else 1)
    grads = dot(d_pairs, pooled, 0, 1 if turn else 0, precision=HIGH)
    for m in range(2):
        pair_out[m] = grads[m * latent : (m + 1) * latent]

    landed(("done",), out.at[0 : (tm - 1) * mine])
    remote(out.at[0 : (tm - 1) * mine], out.at[0 : (tm - 1) * mine], ("done",), i, t).wait_send()
    settle(started)
    assert len(tags) <= send.shape[0], len(tags)


def write_out(grad, pair, step, grad_out, pair_out, step_out, sem):
    chunk = grad.shape[0] // 4
    parts = [pl.ds(n * chunk, chunk) for n in range(4)]
    copies = [
        pltpu.make_async_copy(src, dst, sem.at[n])
        for n, (src, dst) in enumerate(
            [(grad.at[part], grad_out.at[part]) for part in parts] + [(pair, pair_out), (step, step_out)]
        )
    ]
    for copy in copies:
        copy.start()
    for copy in copies:
        copy.wait()


def local(dp, tm, tokens, gain, w_qkv, w_out, w_pair, codebook, codes):
    patches, width = tokens.shape[2:]
    rows = w_qkv.shape[0]
    latent, n_codes = w_pair.shape[2], codebook.shape[0]
    both = 2 * latent
    fp = -(-tm // 8) * 8
    sr = -(-2 * tm // 8) * 8
    lanes = tm * (width // HEAD_DIM)
    pieces = width // 256
    assert rows <= LANES and 2 * both <= LANES and both + n_codes <= LANES
    slab = (rows, dp * tm) if rows % LANES else (dp * tm, rows)
    chips = dp // 2
    tags = (26 if chips == 4 else 2 * dp + 4) + 2 * chips + 8
    vmem = pl.BlockSpec(memory_space=pltpu.VMEM)
    hbm = pl.BlockSpec(memory_space=pltpu.HBM)
    grad, pair, step = pl.pallas_call(
        functools.partial(kernel, (dp, tm, rows, patches, width, latent, n_codes, pieces)),
        out_shape=(
            pltpu.VMEM((patches, width), BF16),
            pltpu.VMEM((2, latent, width), F32),
            pltpu.VMEM((n_codes, latent), F32),
        ),
        in_specs=[hbm] * 7,
        out_specs=(vmem, vmem, vmem),
        scratch_shapes=[
            pltpu.VMEM((dp * rows, 3 * width), BF16),
            pltpu.VMEM((3 * width, dp * rows), BF16),
            pltpu.VMEM((rows, width), BF16),
            pltpu.VMEM((both, width), F32),
            pltpu.VMEM((width,), BF16),
            pltpu.VMEM((n_codes, latent), F32),
            pltpu.SMEM((1, 1, 1), jnp.int32),
            pltpu.VMEM((patches, width), BF16),
            pltpu.VMEM((patches, width), BF16),
            pltpu.VMEM((patches, LANES), F32),
            pltpu.VMEM((patches if 2 * rows % LANES == 0 else 8, 3 * width), F32),
            pltpu.VMEM((patches, 3 * width), BF16),
            pltpu.VMEM((tm * width, lanes), BF16),
            pltpu.VMEM((lanes, width), BF16),
            pltpu.VMEM((patches, lanes), F32),
            pltpu.VMEM((patches, lanes), F32),
            pltpu.VMEM((patches, lanes), BF16),
            pltpu.VMEM((lanes, width), BF16),
            pltpu.VMEM((patches, lanes), F32),
            pltpu.VMEM((patches, LANES), F32),
            pltpu.VMEM((patches, 3 * width), BF16),
            pltpu.VMEM((patches, width), BF16),
            pltpu.VMEM((fp, width), F32),
            pltpu.VMEM((fp, width), F32),
            pltpu.VMEM((3 * both, width), BF16),
            pltpu.VMEM((3 * both, width), BF16),
            pltpu.VMEM((dp, both, rows), F32),
            pltpu.VMEM((fp, LANES), F32),
            pltpu.VMEM((tm, fp, LANES), F32),
            pltpu.VMEM((sr, width), F32),
            pltpu.VMEM((tm, sr, width), F32),
            pltpu.VMEM((dp, 2, sr, LANES), F32),
            pltpu.VMEM((dp, 2, sr, LANES), F32),
            pltpu.VMEM((dp, *slab), F32),
            pltpu.VMEM((dp, *slab), F32),
            pltpu.VMEM((dp, *slab), F32),
            pltpu.SemaphoreType.DMA((tags,)),
            pltpu.SemaphoreType.DMA((tags,)),
            pltpu.SemaphoreType.DMA((10,)),
        ],
        compiler_params=pltpu.CompilerParams(
            collective_id=0, has_side_effects=True, vmem_limit_bytes=60000 * 1024
        ),
    )(
        tokens.reshape(patches, width), gain, w_qkv, w_out, w_pair.swapaxes(1, 2).reshape(both, width), codebook,
        codes,
    )
    made = (grad, pair, step)
    grad, pair, step = pl.pallas_call(
        write_out,
        out_shape=tuple(jax.ShapeDtypeStruct(v.shape, v.dtype) for v in made),
        in_specs=[vmem] * 3,
        out_specs=(hbm, hbm, hbm),
        scratch_shapes=[pltpu.SemaphoreType.DMA((6,))],
        compiler_params=pltpu.CompilerParams(vmem_limit_bytes=4096 * 1024),
    )(*made)
    return grad.reshape(tokens.shape), pair.swapaxes(1, 2), step


def solution(mesh):
    placed = (
        P("dp", "tm", None, None),
        P(),
        P("dp", None),
        P("dp", None),
        P(),
        P(),
        P("dp", "tm", None),
    )
    return jax.shard_map(
        functools.partial(local, mesh.shape["dp"], mesh.shape["tm"]),
        mesh=mesh,
        in_specs=placed,
        out_specs=(P("dp", "tm", None, None), P(), P()),
        check_vma=False,
    )
```
